32 devices in a mesh: clip: 2 (over y), rows: 8 (over z, x), tm: 2 (over core).
Axes of the slice: x: 2, y: 2, z: 4, core: 2. Of those that a mesh axis runs over, the one named last changes fastest.
Arguments:
- latent: bfloat16 [8, 8, 64, 192], P(('clip', 'tm'), 'rows'), parts along dimension 0, may hold values from -18 to 18
- gain_first: bfloat16 [192], replicated, may hold values from 0.099609375 to 1.8984375
- conv_first: bfloat16 [3, 3, 3, 192, 192], replicated, may hold values from -0.078125 to 0.078125
- gain_second: bfloat16 [192], replicated, may hold values from 0.099609375 to 1.8984375
- conv_second: bfloat16 [3, 3, 3, 192, 192], replicated, may hold values from -0.078125 to 0.078125
- conv_up: bfloat16 [3, 3, 96, 192], replicated, may hold values from -0.15625 to 0.15625
Outputs:
- decoded: bfloat16 [8, 16, 96, 128], P(('clip', 'tm'), 'rows'), parts along dimension 0
- peaks: float32 [6, 192], P('clip'), parts along dimension 0
The draws below stay inside these ranges and needn't reach their ends.
There are 2 independent parts, one for each index of `clip`. The reference program is written for one: setup_inputs(seed, part) draws one part's arguments, and reference() takes and returns one part's arrays. A program takes and returns all parts, laid end to end along the dimension named above; an argument that names none is the same for every part. Nothing has to cross between parts.
All inputs are finite; a program needn't handle non-finite values.
Results may differ from the reference program's by a relative error of at most 0.0085.
Values may be sent and summed in bfloat16 or wider, within the bound.
A program may use at most 64 MiB of HBM per device.

```python
import math
import jax
import jax.numpy as jnp
from jax import lax

C = 192
C2 = 96
COLS = 64
FRAMES = 4
ROWS = 8


def draw_latent(key, part):
    base_key = jax.random.fold_in(key, 11)
    noise_key, spread_key = jax.random.split(base_key)
    spread = jnp.exp(jax.random.uniform(spread_key, (1, ROWS, 1, C), jnp.float32, math.log(0.3), math.log(3.0)))
    rising = 0.5 + jnp.arange(ROWS, dtype=jnp.float32).reshape(1, ROWS, 1, 1) / ROWS
    noise = jnp.clip(jax.random.normal(noise_key, (FRAMES, ROWS, COLS, C), jnp.float32), -4.0, 4.0)
    return (noise * spread * rising).astype(jnp.bfloat16)


def scatter_about(own_key, dims, deviation, most, kind=jnp.bfloat16):
    entries = jax.random.normal(own_key, dims, jnp.float32) * deviation
    return jnp.minimum(jnp.maximum(entries, -most), most).astype(kind)


def setup_inputs(seed: int = 0, part: int = 0) -> dict:
    splits = jax.random.split(jax.random.key(seed), 7)
    part_splits = jax.random.split(jax.random.fold_in(splits[6], part), 7)
    latent = draw_latent(jax.random.fold_in(jax.random.fold_in(splits[6], part), 71), part)
    gain_first = jnp.clip(1.0 + 0.18 * jax.random.normal(splits[1], (C,), jnp.float32), 0.099609375, 1.8984375).astype(jnp.bfloat16)
    conv_first = scatter_about(splits[2], (3, 3, 3, C, C), (27 * C) ** -0.5, 0.078125)
    gain_second = jnp.clip(1.0 + 0.18 * jax.random.normal(splits[3], (C,), jnp.float32), 0.099609375, 1.8984375).astype(jnp.bfloat16)
    conv_second = scatter_about(splits[4], (3, 3, 3, C, C), (27 * C) ** -0.5, 0.078125)
    conv_up = scatter_about(splits[5], (3, 3, C2, C), (9 * C) ** -0.5, 0.15625)
    return {"latent": latent, "gain_first": gain_first, "conv_first": conv_first, "gain_second": gain_second, "conv_second": conv_second, "conv_up": conv_up}


def rms_norm(values, gain):
    floats = values.astype(jnp.float32)
    scale = lax.rsqrt(lax.optimization_barrier(jnp.mean(floats * floats, axis=-1, keepdims=True)) + 1e-06)
    return floats * scale * gain.astype(jnp.float32)

def causal_taps(extended, weights, frame_count, row_count, col_count):
    channels = extended.shape[-1]
    total = jnp.zeros((frame_count * row_count * col_count, weights.shape[-1]), jnp.float32)
    for time_tap in range(3):
        for row_tap in range(3):
            sliced = extended[time_tap:time_tap + frame_count, row_tap:row_tap + row_count]
            stacked = jnp.concatenate([sliced[:, :, col_tap:col_tap + col_count] for col_tap in range(3)], axis=-1)
            matrix = weights[time_tap, row_tap].reshape(3 * channels, weights.shape[-1])
            total = total + jnp.dot(stacked.reshape(-1, 3 * channels), matrix, preferred_element_type=jnp.float32)
    return total.reshape(frame_count, row_count, col_count, weights.shape[-1])

def plane_taps(wide_padded, conv_up, row_count, col_count):
    channels = wide_padded.shape[-1]
    frame_count = wide_padded.shape[0]
    total = jnp.zeros((frame_count * row_count * col_count, conv_up.shape[2]), jnp.float32)
    for row_tap in range(3):
        sliced = wide_padded[:, row_tap:row_tap + row_count]
        stacked = jnp.concatenate([sliced[:, :, col_tap:col_tap + col_count] for col_tap in range(3)], axis=-1)
        matrix = jnp.transpose(conv_up[row_tap], (0, 2, 1)).reshape(3 * channels, conv_up.shape[2])
        total = total + jnp.dot(stacked.reshape(-1, 3 * channels), matrix, preferred_element_type=jnp.float32)
    output = total.reshape(frame_count, row_count, col_count, conv_up.shape[2])
    return jnp.transpose(output, (0, 1, 3, 2)).astype(jnp.bfloat16)

def channel_peak(values):
    return lax.optimization_barrier(jnp.max(jnp.abs(values).astype(jnp.float32), axis=(0, 1, 2)))

def causal_whole(values, weights):
    frame_count, row_count, col_count = (values.shape[0], values.shape[1], values.shape[2])
    extended = jnp.pad(values, ((2, 0), (1, 1), (1, 1), (0, 0)))
    return causal_taps(extended, weights, frame_count, row_count, col_count)

def reference(latent, gain_first, conv_first, gain_second, conv_second, conv_up):
    first = jax.nn.silu(rms_norm(latent, gain_first)).astype(jnp.bfloat16)
    hidden = causal_whole(first, conv_first).astype(jnp.bfloat16)
    second = jax.nn.silu(rms_norm(hidden, gain_second)).astype(jnp.bfloat16)
    merged = (latent.astype(jnp.float32) + causal_whole(second, conv_second)).astype(jnp.bfloat16)
    row_count, col_count = (merged.shape[1], merged.shape[2])

    def one_frame(frame):
        wide = jnp.repeat(jnp.repeat(frame[None], 2, axis=1), 2, axis=2)
        wide = jnp.pad(wide, ((0, 0), (1, 1), (1, 1), (0, 0)))
        return plane_taps(wide, conv_up, 2 * row_count, 2 * col_count)[0]
    decoded = lax.map(one_frame, merged)
    peaks = jnp.stack([channel_peak(first), channel_peak(second), channel_peak(merged)], axis=0)
    return (decoded, peaks)
```

```python
import functools

import jax
import jax.numpy as jnp
from jax import lax
from jax.experimental import pallas as pl
from jax.experimental.pallas import tpu as pltpu
from jax.sharding import PartitionSpec as P

MESH = pl.DeviceIdType.MESH
BF16 = jnp.bfloat16
F32 = jnp.float32
REACH = 2
LANES = 128


def normed_silu(values, gain):
    scale = lax.rsqrt(jnp.mean(values * values, axis=-1, keepdims=True) + 1e-06)
    u = values * scale * gain
    return u / (1.0 + jnp.exp(-u))


def peak_of(values):
    return jnp.max(jnp.abs(values), axis=0, keepdims=True)


def dot(a, b):
    return jnp.dot(a, b, preferred_element_type=F32)


def dot_nt(a, b):
    return lax.dot_general(a, b, (((1,), (1,)), ((), ())), preferred_element_type=F32)


def packed(values, cols):
    low = values[:, 0:LANES].reshape(2, cols, LANES)
    high = jnp.concatenate([values[0:cols, LANES:], values[cols:, LANES:]], axis=1)
    return jnp.concatenate([low, high[None]], axis=0).astype(BF16)


def frames_of(buf):
    high = buf[2]
    turned = pltpu.roll(high.astype(F32), LANES // 2, 1).astype(BF16)
    return jnp.concatenate([buf[0], high], axis=1), jnp.concatenate([buf[1], turned], axis=1)


def finish(dec_in, peaks_in, dec_out, peaks_out, sem):
    copies = [
        pltpu.make_async_copy(dec_in, dec_out, sem.at[0]),
        pltpu.make_async_copy(peaks_in, peaks_out, sem.at[1]),
    ]
    for copy in copies:
        copy.start()
    for copy in copies:
        copy.wait()


def kernel(
    R, T, lat_hbm, g1_hbm, w1_hbm, g2_hbm, w2_hbm, up_hbm, dec_ref, peaks_ref,
    lat, g1, g2, rows_in, hist, acc, second, past, w1, w2, up, merged,
    pk1_send, pk1_recv, pk2_send, pk2_recv,
    load_sem, x1_send, x1_recv, rl_send, rl_recv, s_send, s_recv, x3_send, x3_recv,
    pk1_ssem, pk1_rsem, pk2_ssem, pk2_rsem, known, spread,
):
    r = lax.axis_index("rows")
    t = lax.axis_index("tm")
    n = R * T
    me = r * T + t
    frames, cols, C = lat.shape
    width = frames * cols

    def there(d):
        return jnp.logical_and(r + d >= 0, r + d < R)

    barrier = pltpu.get_barrier_semaphore()
    near = [(d, e) for d in range(-REACH, REACH + 1) for e in range(T) if (d, e) != (0, 0)]

    def greet(d, e):
        pl.semaphore_signal(
            barrier, inc=1, device_id={"rows": r + d, "tm": lax.rem(t + e, T)}, device_id_type=MESH
        )

    loads = [
        pltpu.make_async_copy(lat_hbm, lat, load_sem.at[0]),
        pltpu.make_async_copy(g1_hbm, g1, load_sem.at[1]),
        pltpu.make_async_copy(g2_hbm, g2, load_sem.at[2]),
        pltpu.make_async_copy(w1_hbm, w1.at[:, 0:C, :], load_sem.at[3]),
        pltpu.make_async_copy(w2_hbm, w2.at[:, 0:C, :], load_sem.at[4]),
        pltpu.make_async_copy(up_hbm, up, load_sem.at[5]),
    ]
    loads[0].start()
    loads[1].start()
    for d, e in near:
        pl.when(there(d))(functools.partial(greet, d, e))
    for copy in loads[2:]:
        copy.start()

    @pl.when(r == 0)
    def _():
        merged[0] = jnp.zeros_like(merged[0])

    @pl.when(r == R - 1)
    def _():
        merged[2] = jnp.zeros_like(merged[2])

    pad = w1.shape[1] - C
    w1[:, C:, :] = jnp.zeros((w1.shape[0], pad, C), BF16)
    w2[:, C:, :] = jnp.zeros((w2.shape[0], pad, C), BF16)
    pk1_send[...] = jnp.zeros_like(pk1_send)
    pk2_send[...] = jnp.zeros_like(pk2_send)

    q = lax.broadcasted_iota(jnp.int32, (2 * width, 2 * width), 0)
    o = lax.broadcasted_iota(jnp.int32, (2 * width, 2 * width), 1)
    frame = lax.rem(lax.div(q, cols), frames)
    target = frame * (2 * cols) + 2 * lax.rem(q, cols) + lax.div(q, width)
    spread[...] = jnp.where(o == target, 1.0, 0.0).astype(BF16)

    loads[0].wait()
    loads[1].wait()
    gain1 = g1[...].astype(F32).reshape(1, C)
    own_first = normed_silu(lat[...].astype(F32).reshape(width, C), gain1)
    rows_in[REACH] = packed(own_first, cols)

    rows_near = 1 + jnp.minimum(r, REACH) + jnp.minimum(R - 1 - r, REACH)
    pl.semaphore_wait(barrier, rows_near * T - 1)

    side = 1 - 2 * lax.rem(r, 2)

    def row_copy(d):
        slot = REACH - d
        return pltpu.make_async_remote_copy(
            src_ref=rows_in.at[REACH], dst_ref=rows_in.at[slot], send_sem=x1_send.at[slot],
            recv_sem=x1_recv.at[slot], device_id={"rows": r + d}, device_id_type=MESH,
        )

    for d in (-side, side, 2 * side, -2 * side):
        pl.when(there(d))(lambda d=d: row_copy(d).start())

    def relay(slot):
        return pltpu.make_async_remote_copy(
            src_ref=rows_in.at[slot], dst_ref=hist.at[slot], send_sem=rl_send.at[slot],
            recv_sem=rl_recv.at[slot], device_id={"tm": t + 1}, device_id_type=MESH,
        )

    gives = t < T - 1
    takes = t > 0
    pl.when(gives)(lambda: relay(REACH).start())

    stages = [REACH << i for i in range(R.bit_length()) if (REACH << i) < R - 1]

    def tell(i):
        for way, d in enumerate((stages[i], -stages[i])):
            pl.when(there(d))(
                lambda way=way, d=d: pl.semaphore_signal(
                    known.at[i, way], inc=1, device_id={"rows": r + d}, device_id_type=MESH
                )
            )

    def hear(i):
        for way, d in enumerate((stages[i], -stages[i])):
            pl.when(there(-d))(lambda way=way: pl.semaphore_wait(known.at[i, way], 1))

    if stages:
        tell(0)

    def put_peak(ref, i, row):
        ref[2 * i : 2 * i + 1, :] = row[:, 0:LANES]
        ref[2 * i + 1 : 2 * i + 2, 0 : C - LANES] = row[:, LANES:C]

    put_peak(pk1_send, 0, peak_of(own_first.astype(BF16).astype(F32)))

    def contribute(buf, pairs, past_frames, fresh=False):
        f0, f1 = frames_of(buf)
        both = jnp.concatenate([f0, f1], axis=0)
        tap = 0 if past_frames else 2
        for at, j in pairs:
            for k in range(3):
                main = dot(both, w1[(tap * 3 + j) * 3 + k])
                extra = dot(f1 if past_frames else f0, w1[(3 + j) * 3 + k])
                early, late = main[0:cols], main[cols:]
                if past_frames:
                    early = early + extra
                else:
                    late = late + extra
                if fresh:
                    acc[k, at, 0:cols] = early
                    acc[k, at, cols:] = late
                else:
                    acc[k, at, 0:cols] += early
                    acc[k, at, cols:] += late

    own_pairs = [(0, 2), (1, 1), (2, 0)]

    def pairs_of(s, far):
        return [(1 + s, 1 + s)] if far else [(1, 1 + s), (1 + s, 1)]

    loads[3].wait()
    contribute(rows_in.at[REACH], own_pairs, False, fresh=True)

    @pl.when(takes)
    def _():
        relay(REACH).wait_recv()
        contribute(hist.at[REACH], own_pairs, True)

    steps = [(side, False), (side, True), (-side, True), (-side, False)]

    def fresh_row(s, far):
        d = 2 * s if far else s
        slot = REACH + d

        @pl.when(there(d))
        def _():
            row_copy(-d).wait_recv()
            pl.when(gives)(lambda: relay(slot).start())
            contribute(rows_in.at[slot], pairs_of(s, far), False)

    def past_row(s, far):
        d = 2 * s if far else s
        slot = REACH + d

        @pl.when(jnp.logical_and(takes, there(d)))
        def _():
            relay(slot).wait_recv()
            contribute(hist.at[slot], pairs_of(s, far), True)

    fresh_row(*steps[0])
    fresh_row(*steps[1])
    past_row(*steps[0])
    fresh_row(*steps[2])
    past_row(*steps[1])
    fresh_row(*steps[3])
    past_row(*steps[2])
    past_row(*steps[3])

    for i in range(1, len(stages)):
        hear(i - 1)
        tell(i)

    lane0 = lax.rem(lax.broadcasted_iota(jnp.int32, (width, 1), 0), cols)

    def shifted_sum(left, middle, right):
        left = jnp.where(lane0 == 0, 0.0, pltpu.roll(left, 1, 0))
        right = jnp.where(lane0 == cols - 1, 0.0, pltpu.roll(right, width - 1, 0))
        return left + middle + right

    loads[2].wait()
    gain2 = g2[...].astype(F32).reshape(1, C)
    for at in range(3):
        hidden = shifted_sum(acc[0, at], acc[1, at], acc[2, at]).astype(BF16).astype(F32)
        values = normed_silu(hidden, gain2)
        if at != 1:
            values = jnp.where(there(at - 1), values, 0.0)
        else:
            put_peak(pk1_send, 1, peak_of(values.astype(BF16).astype(F32)))
        second[at] = packed(values, cols)

    def hand_on():
        return pltpu.make_async_remote_copy(
            src_ref=second, dst_ref=past,
            send_sem=s_send, recv_sem=s_recv, device_id={"tm": t + 1}, device_id_type=MESH,
        )

    pl.when(gives)(lambda: hand_on().start())

    if stages:
        hear(len(stages) - 1)

    def peer_of(i):
        p = jnp.where(2 * r >= R, i, n - 2 - i)
        return jnp.where(p >= me, p + 1, p)

    def peak_copy(src, dst, ssem, rsem, peer, owner):
        return pltpu.make_async_remote_copy(
            src_ref=src, dst_ref=dst.at[owner], send_sem=ssem.at[peer], recv_sem=rsem.at[owner],
            device_id={"rows": peer // T, "tm": lax.rem(peer, T)}, device_id_type=MESH,
        )

    def send_peaks(src, dst, ssem, rsem):
        def step(i, carry):
            peak_copy(src, dst, ssem, rsem, peer_of(i), me).start()
            return carry

        lax.fori_loop(0, n - 1, step, 0, unroll=n <= 16)

    def take_peaks(src, dst, ssem, rsem):
        def step(i, best):
            peer = peer_of(n - 2 - i)
            peak_copy(src, dst, ssem, rsem, peer, peer).wait_recv()
            return jnp.maximum(best, dst[peer])

        return lax.fori_loop(0, n - 1, step, src[...], unroll=n <= 16)

    def end_peaks(src, dst, ssem, rsem):
        def step(i, carry):
            peak_copy(src, dst, ssem, rsem, peer_of(i), me).wait_send()
            return carry

        lax.fori_loop(0, n - 1, step, 0, unroll=n <= 16)

    early = (pk1_send, pk1_recv, pk1_ssem, pk1_rsem)
    last = (pk2_send, pk2_recv, pk2_ssem, pk2_rsem)
    send_peaks(*early)

    loads[4].wait()

    def second_part(buf, past_frames):
        pieces = [frames_of(buf.at[j]) for j in range(3)]
        f0 = jnp.concatenate([piece[0] for piece in pieces], axis=1)
        f1 = jnp.concatenate([piece[1] for piece in pieces], axis=1)
        both = jnp.concatenate([f0, f1], axis=0)
        tap = 0 if past_frames else 2
        for k in range(3):
            main = dot(both, jnp.concatenate([w2[(tap * 3 + j) * 3 + k] for j in range(3)], axis=0))
            extra = dot(
                f1 if past_frames else f0,
                jnp.concatenate([w2[(3 + j) * 3 + k] for j in range(3)], axis=0),
            )
            early, late = main[0:cols], main[cols:]
            if past_frames:
                acc[k, 0, 0:cols] += early + extra
                acc[k, 0, cols:] += late
            else:
                acc[k, 0, 0:cols] = early
                acc[k, 0, cols:] = late + extra

    second_part(second, False)

    @pl.when(takes)
    def _():
        hand_on().wait_recv()
        second_part(past, True)

    block = lat[...].astype(F32).reshape(width, C) + shifted_sum(acc[0, 0], acc[1, 0], acc[2, 0])
    block = block.astype(BF16)
    wide_block = block.astype(F32)
    merged[1] = packed(wide_block, cols)
    put_peak(pk2_send, 0, peak_of(wide_block))
    send_peaks(*last)

    def edge_copy(d):
        slot = 1 - d
        return pltpu.make_async_remote_copy(
            src_ref=merged.at[1], dst_ref=merged.at[slot], send_sem=x3_send.at[slot],
            recv_sem=x3_recv.at[slot], device_id={"rows": r + d}, device_id_type=MESH,
        )

    for d in (-side, side):
        pl.when(there(d))(lambda d=d: edge_copy(d).start())

    loads[5].wait()
    C2 = dec_ref.shape[2]
    own = dot_nt(up[...], block).reshape(3, 3, C2, width)
    upper = own[1] + own[2]
    lower = own[0] + own[1]

    def edge_row(slot):
        f0, f1 = frames_of(merged.at[slot])
        return jnp.concatenate([f0, f1], axis=0)[:, 0:C]

    for d in (side, -side):
        pl.when(there(d))(lambda d=d: edge_copy(-d).wait_recv())
    upper = upper + dot_nt(up[0 : 3 * C2], edge_row(0)).reshape(3, C2, width)
    lower = lower + dot_nt(up[6 * C2 :], edge_row(2)).reshape(3, C2, width)
    lane = lax.rem(lax.broadcasted_iota(jnp.int32, (C2, width), 1), cols)

    def columns(sums):
        from_left = jnp.where(lane == 0, 0.0, pltpu.roll(sums[0], 1, 1))
        from_right = jnp.where(lane == cols - 1, 0.0, pltpu.roll(sums[2], width - 1, 1))
        even = from_left + sums[1] + sums[2]
        odd = sums[0] + sums[1] + from_right
        return jnp.concatenate([even, odd], axis=1).astype(BF16)

    narrow = jnp.concatenate([columns(upper), columns(lower)], axis=0)
    wide = dot(narrow, spread[...]).astype(BF16)
    for f in range(frames):
        for j in range(2):
            dec_ref[f, j] = wide[j * C2 : (j + 1) * C2, f * 2 * cols : (f + 1) * 2 * cols]

    best = take_peaks(*early)
    for i in range(2):
        peaks_ref[i : i + 1, 0:LANES] = best[2 * i : 2 * i + 1, :]
        peaks_ref[i : i + 1, LANES:C] = best[2 * i + 1 : 2 * i + 2, 0 : C - LANES]
    best = take_peaks(*last)
    peaks_ref[2:3, 0:LANES] = best[0:1, :]
    peaks_ref[2:3, LANES:C] = best[1:2, 0 : C - LANES]

    end_peaks(*early)
    end_peaks(*last)
    for d in (1, -1, 2, -2):
        pl.when(there(d))(lambda d=d: row_copy(d).wait_send())
    for d in (1, -1):
        pl.when(there(d))(lambda d=d: edge_copy(d).wait_send())

    @pl.when(gives)
    def _():
        for d in (0, 1, -1, 2, -2):
            pl.when(there(d))(lambda d=d: relay(REACH + d).wait_send())
        hand_on().wait_send()


def per_device(latent, gain_first, conv_first, gain_second, conv_second, conv_up):
    frames, rows, cols, C = latent.shape
    R, T = lax.axis_size("rows"), lax.axis_size("tm")
    C2 = conv_up.shape[2]
    n = R * T
    if rows != 1 or frames != 2 or 2 * C != 3 * LANES:
        raise ValueError("unsupported block")
    depth = 2 * LANES
    taps = conv_first.shape[0] * conv_first.shape[1] * conv_first.shape[2]
    vmem = pl.BlockSpec(memory_space=pltpu.VMEM)
    hbm = pl.BlockSpec(memory_space=pltpu.HBM)
    dma = pltpu.SemaphoreType.DMA
    span = 2 * REACH + 1
    width = frames * cols
    decoded, peaks = pl.pallas_call(
        functools.partial(kernel, R, T),
        out_shape=(
            pltpu.VMEM((frames, 2 * rows, C2, 2 * cols), BF16),
            pltpu.VMEM((3, C), F32),
        ),
        in_specs=[hbm] * 6,
        out_specs=(vmem, vmem),
        scratch_shapes=[
            pltpu.VMEM((frames, cols, C), BF16),
            pltpu.VMEM((C,), BF16),
            pltpu.VMEM((C,), BF16),
            pltpu.VMEM((span, 3, cols, LANES), BF16),
            pltpu.VMEM((span, 3, cols, LANES), BF16),
            pltpu.VMEM((3, 3, width, C), F32),
            pltpu.VMEM((3, 3, cols, LANES), BF16),
            pltpu.VMEM((3, 3, cols, LANES), BF16),
            pltpu.VMEM((taps, depth, C), BF16),
            pltpu.VMEM((taps, depth, C), BF16),
            pltpu.VMEM((9 * C2, C), BF16),
            pltpu.VMEM((3, 3, cols, LANES), BF16),
            pltpu.VMEM((4, LANES), F32),
            pltpu.VMEM((n, 4, LANES), F32),
            pltpu.VMEM((2, LANES), F32),
            pltpu.VMEM((n, 2, LANES), F32),
            dma((6,)),
            dma((span,)),
            dma((span,)),
            dma((span,)),
            dma((span,)),
            dma,
            dma,
            dma((3,)),
            dma((3,)),
            dma((n,)),
            dma((n,)),
            dma((n,)),
            dma((n,)),
            pltpu.SemaphoreType.REGULAR((R.bit_length(), 2)),
            pltpu.VMEM((2 * width, 2 * width), BF16),
        ],
        compiler_params=pltpu.CompilerParams(collective_id=0, has_side_effects=True, vmem_limit_bytes=54 * 2**20),
    )(
        latent.reshape(frames, cols, C),
        gain_first,
        conv_first.reshape(taps, C, C),
        gain_second,
        conv_second.reshape(taps, C, C),
        conv_up.reshape(9 * C2, C),
    )
    return pl.pallas_call(
        finish,
        out_shape=(
            jax.ShapeDtypeStruct(decoded.shape, BF16),
            jax.ShapeDtypeStruct(peaks.shape, F32),
        ),
        in_specs=[vmem, vmem],
        out_specs=(hbm, hbm),
        scratch_shapes=[dma((2,))],
        compiler_params=pltpu.CompilerParams(vmem_limit_bytes=2**20),
    )(decoded, peaks)


def solution(mesh):
    return jax.shard_map(
        per_device,
        mesh=mesh,
        in_specs=(P(("clip", "tm"), "rows", None, None), P(), P(), P(), P(), P()),
        out_specs=(P(("clip", "tm"), "rows", None, None), P("clip", None)),
        check_vma=False,
    )
```

```python
import functools

import jax
import jax.numpy as jnp
from jax import lax
from jax.experimental import pallas as pl
from jax.experimental.pallas import tpu as pltpu
from jax.sharding import PartitionSpec as P

MESH = pl.DeviceIdType.MESH
BF16 = jnp.bfloat16
F32 = jnp.float32
REACH = 2
LANES = 128


def normed_silu(values, gain):
    scale = lax.rsqrt(jnp.mean(values * values, axis=-1, keepdims=True) + 1e-06)
    u = values * scale * gain
    return u / (1.0 + jnp.exp(-u))


def peak_of(values):
    return jnp.max(jnp.abs(values), axis=0, keepdims=True)


def dot(a, b):
    return jnp.dot(a, b, preferred_element_type=F32)


def dot_nt(a, b):
    return lax.dot_general(a, b, (((1,), (1,)), ((), ())), preferred_element_type=F32)


def packed(values, cols):
    low = values[:, 0:LANES].reshape(2, cols, LANES)
    high = jnp.concatenate([values[0:cols, LANES:], values[cols:, LANES:]], axis=1)
    return jnp.concatenate([low, high[None]], axis=0).astype(BF16)


def frames_of(buf):
    high = buf[2]
    turned = pltpu.roll(high.astype(F32), LANES // 2, 1).astype(BF16)
    return jnp.concatenate([buf[0], high], axis=1), jnp.concatenate([buf[1], turned], axis=1)


def finish(dec_in, peaks_in, dec_out, peaks_out, sem):
    copies = [
        pltpu.make_async_copy(dec_in, dec_out, sem.at[0]),
        pltpu.make_async_copy(peaks_in, peaks_out, sem.at[1]),
    ]
    for copy in copies:
        copy.start()
    for copy in copies:
        copy.wait()


def kernel(
    R, T, lat_hbm, g1_hbm, w1_hbm, g2_hbm, w2_hbm, up_hbm, dec_ref, peaks_ref,
    lat, g1, g2, rows_in, hist, acc, mix, second, past, w1, w2, up, merged,
    pk1_send, pk1_recv, pk2_send, pk2_recv, pk_second,
    load_sem, x1_send, x1_recv, rl_send, rl_recv, s_send, s_recv, x3_send, x3_recv,
    pk1_ssem, pk1_rsem, pk2_ssem, pk2_rsem, known, spread,
):
    r = lax.axis_index("rows")
    t = lax.axis_index("tm")
    n = R * T
    me = r * T + t
    frames, cols, C = lat.shape
    width = frames * cols

    def there(d):
        return jnp.logical_and(r + d >= 0, r + d < R)

    barrier = pltpu.get_barrier_semaphore()
    near = [(d, e) for d in range(-REACH, REACH + 1) for e in range(T) if (d, e) != (0, 0)]

    def greet(d, e):
        pl.semaphore_signal(
            barrier, inc=1, device_id={"rows": r + d, "tm": lax.rem(t + e, T)}, device_id_type=MESH
        )

    loads = [
        pltpu.make_async_copy(lat_hbm, lat, load_sem.at[0]),
        pltpu.make_async_copy(g1_hbm, g1, load_sem.at[1]),
        pltpu.make_async_copy(g2_hbm, g2, load_sem.at[2]),
        pltpu.make_async_copy(w1_hbm, w1.at[:, 0:C, :], load_sem.at[3]),
        pltpu.make_async_copy(w2_hbm, w2.at[:, 0:C, :], load_sem.at[4]),
        pltpu.make_async_copy(up_hbm, up, load_sem.at[5]),
    ]
    loads[0].start()
    loads[1].start()
    for d, e in near:
        pl.when(there(d))(functools.partial(greet, d, e))
    loads[3].start()
    loads[2].start()

    @pl.when(r == 0)
    def _():
        merged[0] = jnp.zeros_like(merged[0])

    @pl.when(r == R - 1)
    def _():
        merged[2] = jnp.zeros_like(merged[2])

    for d in (-2, -1, 1, 2):

        @pl.when(jnp.logical_not(there(d)))
        def _(d=d):
            rows_in[REACH + d] = jnp.zeros_like(rows_in[REACH + d])
            hist[REACH + d] = jnp.zeros_like(hist[REACH + d])
            if abs(d) == 1:
                second[1 + d] = jnp.zeros_like(second[1 + d])

    pad = w1.shape[1] - C
    w1[:, C:, :] = jnp.zeros((w1.shape[0], pad, C), BF16)
    w2[:, C:, :] = jnp.zeros((w2.shape[0], pad, C), BF16)

    q = lax.broadcasted_iota(jnp.int32, (2 * width, 2 * width), 0)
    o = lax.broadcasted_iota(jnp.int32, (2 * width, 2 * width), 1)
    frame = lax.rem(lax.div(q, cols), frames)
    target = frame * (2 * cols) + 2 * lax.rem(q, cols) + lax.div(q, width)
    spread[...] = jnp.where(o == target, 1.0, 0.0).astype(BF16)

    loads[0].wait()
    loads[1].wait()
    gain1 = g1[...].astype(F32).reshape(1, C)
    own_first = normed_silu(lat[...].astype(F32).reshape(width, C), gain1)
    rows_in[REACH] = packed(own_first, cols)

    rows_near = 1 + jnp.minimum(r, REACH) + jnp.minimum(R - 1 - r, REACH)
    pl.semaphore_wait(barrier, rows_near * T - 1)

    side = 1 - 2 * lax.rem(r, 2)

    def row_copy(d):
        slot = REACH - d
        return pltpu.make_async_remote_copy(
            src_ref=rows_in.at[REACH], dst_ref=rows_in.at[slot], send_sem=x1_send.at[slot],
            recv_sem=x1_recv.at[slot], device_id={"rows": r + d}, device_id_type=MESH,
        )

    for d in (-side, side, 2 * side, -2 * side):
        pl.when(there(d))(lambda d=d: row_copy(d).start())

    def relay(slot):
        return pltpu.make_async_remote_copy(
            src_ref=rows_in.at[slot], dst_ref=hist.at[slot], send_sem=rl_send.at[slot],
            recv_sem=rl_recv.at[slot], device_id={"tm": t + 1}, device_id_type=MESH,
        )

    gives = t < T - 1
    takes = t > 0
    pl.when(gives)(lambda: relay(REACH).start())

    stages = [REACH << i for i in range(R.bit_length()) if (REACH << i) < R - 1]

    def tell(i):
        for way, d in enumerate((stages[i], -stages[i])):
            pl.when(there(d))(
                lambda way=way, d=d: pl.semaphore_signal(
                    known.at[i, way], inc=1, device_id={"rows": r + d}, device_id_type=MESH
                )
            )

    def hear(i):
        for way, d in enumerate((stages[i], -stages[i])):
            pl.when(there(-d))(lambda way=way: pl.semaphore_wait(known.at[i, way], 1))

    if stages:
        tell(0)

    def two_rows(row):
        rest = jnp.concatenate([row[:, LANES:C], jnp.zeros((1, 2 * LANES - C), F32)], axis=1)
        return jnp.concatenate([row[:, 0:LANES], rest], axis=0)

    pk1_send[...] = two_rows(peak_of(own_first.astype(BF16).astype(F32))).astype(BF16)

    def contribute(source, past_frames):
        f0, f1 = frames_of(source.at[REACH])
        both = jnp.concatenate([f0, f1], axis=0)
        tap = 0 if past_frames else 2
        for at in range(3):
            j = 2 - at
            for k in range(3):
                main = dot(both, w1[(tap * 3 + j) * 3 + k])
                extra = dot(f1 if past_frames else f0, w1[(3 + j) * 3 + k])
                early, late = main[0:cols], main[cols:]
                if past_frames:
                    acc[k, at, 0:cols] += early + extra
                    acc[k, at, cols:] += late
                else:
                    acc[k, at, 0:cols] = early
                    acc[k, at, cols:] = late + extra

    def contribute_side(source, s, past_frames):
        n0, n1 = frames_of(source.at[REACH + s])
        f0, f1 = frames_of(source.at[REACH + 2 * s])
        near_rows = jnp.concatenate([n0, n1], axis=0)
        all_rows = jnp.concatenate([n0, n1, f0, f1], axis=0)
        near_one, far_one = (n1, f1) if past_frames else (n0, f0)
        ones = jnp.concatenate([near_one, far_one], axis=0)
        tap = 0 if past_frames else 2
        mixed = slice(0, cols) if past_frames else slice(cols, width)
        for k in range(3):
            main = dot(all_rows, w1[(tap * 3 + 1 + s) * 3 + k])
            extra = dot(ones, w1[(3 + 1 + s) * 3 + k])
            acc[k, 1] += main[0:width]
            acc[k, 1, mixed] += extra[0:cols]
            acc[k, 1 + s] += main[width:] + dot(near_rows, w1[(tap * 3 + 1) * 3 + k])
            acc[k, 1 + s, mixed] += extra[cols:] + dot(near_one, w1[(3 + 1) * 3 + k])

    loads[3].wait()
    loads[4].start()
    loads[5].start()
    contribute(rows_in, False)

    def await_row(d):
        @pl.when(there(d))
        def _():
            row_copy(-d).wait_recv()
            pl.when(gives)(lambda: relay(REACH + d).start())

    def await_past(d):
        pl.when(there(d))(lambda: relay(REACH + d).wait_recv())

    lane0 = lax.rem(lax.broadcasted_iota(jnp.int32, (width, 1), 0), cols)

    def shifted_sum(left, middle, right):
        left = jnp.where(lane0 == 0, 0.0, pltpu.roll(left, 1, 0))
        right = jnp.where(lane0 == cols - 1, 0.0, pltpu.roll(right, width - 1, 0))
        return left + middle + right

    def activate(o):
        if isinstance(o, int):
            activate_row(o)
        else:
            pl.when(there(o))(lambda: activate_row(o))

    def activate_row(o):
        at = 1 + o
        hidden = shifted_sum(acc[0, at], acc[1, at], acc[2, at]).astype(BF16).astype(F32)
        values = normed_silu(hidden, gain2)
        if isinstance(o, int):
            pk_second[...] = two_rows(peak_of(values.astype(BF16).astype(F32)))
        second[at] = packed(values, cols)

    def hand_on(o):
        at = 1 + o
        return pltpu.make_async_remote_copy(
            src_ref=second.at[at], dst_ref=past.at[at],
            send_sem=s_send.at[at], recv_sem=s_recv.at[at], device_id={"tm": t + 1}, device_id_type=MESH,
        )

    loads[2].wait()
    gain2 = g2[...].astype(F32).reshape(1, C)

    def second_conv(offsets, fresh, has_past):
        rows = [1 + o for o in offsets]

        def frames_at(source):
            pieces = [frames_of(source.at[j]) for j in rows]
            return [jnp.concatenate([piece[f] for piece in pieces], axis=1) for f in range(2)]

        def taps_at(i, k):
            return [w2[(i * 3 + j) * 3 + k] for j in rows]

        def add(k, part, value):
            if fresh:
                mix[k, part] = value
            else:
                mix[k, part] += value

        f0, f1 = frames_at(second)
        if has_past:
            for o in offsets:
                hand_on(o).wait_recv()
            h0, h1 = frames_at(past)
            early = jnp.concatenate([h0, h1, f0], axis=1)
            late = jnp.concatenate([h1, f0, f1], axis=1)
            lhs = jnp.concatenate([early, late], axis=0)
            for k in range(3):
                taps = [tap for i in range(3) for tap in taps_at(i, k)]
                add(k, slice(0, width), dot(lhs, jnp.concatenate(taps, axis=0)))
        else:
            both = jnp.concatenate([f0, f1], axis=0)
            for k in range(3):
                main = dot(both, jnp.concatenate(taps_at(2, k), axis=0))
                extra = dot(f0, jnp.concatenate(taps_at(1, k), axis=0))
                add(k, slice(0, cols), main[0:cols])
                add(k, slice(cols, width), main[cols:] + extra)

    def meet():
        for i in range(1, len(stages)):
            hear(i - 1)
            tell(i)

    def pass_on(o):
        pl.when(gives)(lambda: hand_on(o).start())

    def peer_of(i):
        p = jnp.where(2 * r >= R, i, n - 2 - i)
        return jnp.where(p >= me, p + 1, p)

    def peak_copy(src, dst, ssem, rsem, peer, owner):
        return pltpu.make_async_remote_copy(
            src_ref=src, dst_ref=dst.at[owner], send_sem=ssem.at[peer], recv_sem=rsem.at[owner],
            device_id={"rows": peer // T, "tm": lax.rem(peer, T)}, device_id_type=MESH,
        )

    def send_peaks(src, dst, ssem, rsem):
        def step(i, carry):
            peak_copy(src, dst, ssem, rsem, peer_of(i), me).start()
            return carry

        lax.fori_loop(0, n - 1, step, 0, unroll=n <= 16)

    def take_peaks(src, dst, ssem, rsem):
        def step(i, best):
            peer = peer_of(n - 2 - i)
            peak_copy(src, dst, ssem, rsem, peer, peer).wait_recv()
            return jnp.maximum(best, dst[peer].astype(F32))

        return lax.fori_loop(0, n - 1, step, src[...].astype(F32), unroll=n <= 16)

    def end_peaks(src, dst, ssem, rsem):
        def step(i, carry):
            peak_copy(src, dst, ssem, rsem, peer_of(i), me).wait_send()
            return carry

        lax.fori_loop(0, n - 1, step, 0, unroll=n <= 16)

    early = (pk1_send, pk1_recv, pk1_ssem, pk1_rsem)
    last = (pk2_send, pk2_recv, pk2_ssem, pk2_rsem)

    def first_peaks():
        if stages:
            hear(len(stages) - 1)
        send_peaks(*early)

    def beside(source, s, past_frames):
        pl.when(there(s))(lambda: contribute_side(source, s, past_frames))

    @pl.when(jnp.logical_not(takes))
    def _():
        await_row(-2)
        meet()
        await_row(side)
        await_row(2)
        beside(rows_in, side, False)
        activate(side)
        pass_on(side)
        await_row(-side)
        beside(rows_in, -side, False)
        activate(0)
        pass_on(0)
        activate(-side)
        pass_on(-side)
        first_peaks()
        loads[4].wait()
        second_conv([-1, 0, 1], True, False)

    @pl.when(takes)
    def _():
        relay(REACH).wait_recv()
        contribute(hist, True)
        meet()
        await_row(-2)
        await_row(side)
        await_row(2)
        beside(rows_in, side, False)
        await_row(-side)
        beside(rows_in, -side, False)
        loads[4].wait()
        first_peaks()
        await_past(-2)
        await_past(side)
        await_past(2)
        beside(hist, side, True)
        activate(side)
        second_conv([side], True, True)
        await_past(-side)
        beside(hist, -side, True)
        activate(0)
        activate(-side)
        second_conv([0, -side], False, True)

    block = lat[...].astype(F32).reshape(width, C) + shifted_sum(mix[0], mix[1], mix[2])
    block = block.astype(BF16)
    wide_block = block.astype(F32)
    merged[1] = packed(wide_block, cols)
    pk2_send[...] = jnp.concatenate([pk_second[...], two_rows(peak_of(wide_block))], axis=0).astype(BF16)
    send_peaks(*last)

    def edge_copy(d):
        slot = 1 - d
        return pltpu.make_async_remote_copy(
            src_ref=merged.at[1], dst_ref=merged.at[slot], send_sem=x3_send.at[slot],
            recv_sem=x3_recv.at[slot], device_id={"rows": r + d}, device_id_type=MESH,
        )

    for d in (-side, side):
        pl.when(there(d))(lambda d=d: edge_copy(d).start())

    loads[5].wait()
    C2 = dec_ref.shape[2]
    own = dot_nt(up[...], block).reshape(3, 3, C2, width)
    upper = own[1] + own[2]
    lower = own[0] + own[1]

    def edge_row(slot):
        f0, f1 = frames_of(merged.at[slot])
        return jnp.concatenate([f0, f1], axis=0)[:, 0:C]

    for d in (side, -side):
        pl.when(there(d))(lambda d=d: edge_copy(-d).wait_recv())
    upper = upper + dot_nt(up[0 : 3 * C2], edge_row(0)).reshape(3, C2, width)
    lower = lower + dot_nt(up[6 * C2 :], edge_row(2)).reshape(3, C2, width)
    lane = lax.rem(lax.broadcasted_iota(jnp.int32, (C2, width), 1), cols)

    def columns(sums):
        from_left = jnp.where(lane == 0, 0.0, pltpu.roll(sums[0], 1, 1))
        from_right = jnp.where(lane == cols - 1, 0.0, pltpu.roll(sums[2], width - 1, 1))
        even = from_left + sums[1] + sums[2]
        odd = sums[0] + sums[1] + from_right
        return jnp.concatenate([even, odd], axis=1).astype(BF16)

    narrow = jnp.concatenate([columns(upper), columns(lower)], axis=0)
    wide = dot(narrow, spread[...]).astype(BF16)
    for f in range(frames):
        for j in range(2):
            dec_ref[f, j] = wide[j * C2 : (j + 1) * C2, f * 2 * cols : (f + 1) * 2 * cols]

    best = jnp.concatenate([take_peaks(*early), take_peaks(*last)], axis=0)
    for i in range(3):
        peaks_ref[i : i + 1, 0:LANES] = best[2 * i : 2 * i + 1, :]
        peaks_ref[i : i + 1, LANES:C] = best[2 * i + 1 : 2 * i + 2, 0 : C - LANES]

    end_peaks(*early)
    end_peaks(*last)
    for d in (1, -1, 2, -2):
        pl.when(there(d))(lambda d=d: row_copy(d).wait_send())
    for d in (1, -1):
        pl.when(there(d))(lambda d=d: edge_copy(d).wait_send())

    @pl.when(gives)
    def _():
        for d in (0, 1, -1, 2, -2):
            pl.when(there(d))(lambda d=d: relay(REACH + d).wait_send())
        for o in (-1, 0, 1):
            hand_on(o).wait_send()


def per_device(latent, gain_first, conv_first, gain_second, conv_second, conv_up):
    frames, rows, cols, C = latent.shape
    R, T = lax.axis_size("rows"), lax.axis_size("tm")
    C2 = conv_up.shape[2]
    n = R * T
    if rows != 1 or frames != 2 or 2 * C != 3 * LANES:
        raise ValueError("unsupported block")
    depth = 2 * LANES
    taps = conv_first.shape[0] * conv_first.shape[1] * conv_first.shape[2]
    vmem = pl.BlockSpec(memory_space=pltpu.VMEM)
    hbm = pl.BlockSpec(memory_space=pltpu.HBM)
    dma = pltpu.SemaphoreType.DMA
    span = 2 * REACH + 1
    width = frames * cols
    decoded, peaks = pl.pallas_call(
        functools.partial(kernel, R, T),
        out_shape=(
            pltpu.VMEM((frames, 2 * rows, C2, 2 * cols), BF16),
            pltpu.VMEM((3, C), F32),
        ),
        in_specs=[hbm] * 6,
        out_specs=(vmem, vmem),
        scratch_shapes=[
            pltpu.VMEM((frames, cols, C), BF16),
            pltpu.VMEM((C,), BF16),
            pltpu.VMEM((C,), BF16),
            pltpu.VMEM((span, 3, cols, LANES), BF16),
            pltpu.VMEM((span, 3, cols, LANES), BF16),
            pltpu.VMEM((3, 3, width, C), F32),
            pltpu.VMEM((3, width, C), F32),
            pltpu.VMEM((3, 3, cols, LANES), BF16),
            pltpu.VMEM((3, 3, cols, LANES), BF16),
            pltpu.VMEM((taps, depth, C), BF16),
            pltpu.VMEM((taps, depth, C), BF16),
            pltpu.VMEM((9 * C2, C), BF16),
            pltpu.VMEM((3, 3, cols, LANES), BF16),
            pltpu.VMEM((2, LANES), BF16),
            pltpu.VMEM((n, 2, LANES), BF16),
            pltpu.VMEM((4, LANES), BF16),
            pltpu.VMEM((n, 4, LANES), BF16),
            pltpu.VMEM((2, LANES), F32),
            dma((6,)),
            dma((span,)),
            dma((span,)),
            dma((span,)),
            dma((span,)),
            dma((3,)),
            dma((3,)),
            dma((3,)),
            dma((3,)),
            dma((n,)),
            dma((n,)),
            dma((n,)),
            dma((n,)),
            pltpu.SemaphoreType.REGULAR((R.bit_length(), 2)),
            pltpu.VMEM((2 * width, 2 * width), BF16),
        ],
        compiler_params=pltpu.CompilerParams(collective_id=0, has_side_effects=True, vmem_limit_bytes=54 * 2**20),
    )(
        latent.reshape(frames, cols, C),
        gain_first,
        conv_first.reshape(taps, C, C),
        gain_second,
        conv_second.reshape(taps, C, C),
        conv_up.reshape(9 * C2, C),
    )
    return pl.pallas_call(
        finish,
        out_shape=(
            jax.ShapeDtypeStruct(decoded.shape, BF16),
            jax.ShapeDtypeStruct(peaks.shape, F32),
        ),
        in_specs=[vmem, vmem],
        out_specs=(hbm, hbm),
        scratch_shapes=[dma((2,))],
        compiler_params=pltpu.CompilerParams(vmem_limit_bytes=2**20),
    )(decoded, peaks)


def solution(mesh):
    return jax.shard_map(
        per_device,
        mesh=mesh,
        in_specs=(P(("clip", "tm"), "rows", None, None), P(), P(), P(), P(), P()),
        out_specs=(P(("clip", "tm"), "rows", None, None), P("clip", None)),
        check_vma=False,
    )
```

```python
import functools

import jax
import jax.numpy as jnp
from jax import lax
from jax.experimental import pallas as pl
from jax.experimental.pallas import tpu as pltpu
from jax.sharding import PartitionSpec as P

MESH = pl.DeviceIdType.MESH
BF16 = jnp.bfloat16
F32 = jnp.float32
REACH = 2
LANES = 128


def stages_of(R):
    return [REACH << i for i in range(R.bit_length()) if (REACH << i) < R - 1]


def normed_silu(values, gain):
    scale = lax.rsqrt(jnp.mean(values * values, axis=-1, keepdims=True) + 1e-06)
    u = values * scale * gain
    return u / (1.0 + jnp.exp(-u))


def peak_of(values):
    return jnp.max(jnp.abs(values), axis=0, keepdims=True)


def dot(a, b):
    return jnp.dot(a, b, preferred_element_type=F32)


def dot_nt(a, b):
    return lax.dot_general(a, b, (((1,), (1,)), ((), ())), preferred_element_type=F32)


def packed(values, cols):
    low = values[:, 0:LANES].reshape(2, cols, LANES)
    high = jnp.concatenate([values[0:cols, LANES:], values[cols:, LANES:]], axis=1)
    return jnp.concatenate([low, high[None]], axis=0).astype(BF16)


def frames_of(buf):
    high = buf[2]
    turned = pltpu.roll(high.astype(F32), LANES // 2, 1).astype(BF16)
    return jnp.concatenate([buf[0], high], axis=1), jnp.concatenate([buf[1], turned], axis=1)


def finish(dec_in, peaks_in, dec_out, peaks_out, sem):
    copies = [
        pltpu.make_async_copy(dec_in, dec_out, sem.at[0]),
        pltpu.make_async_copy(peaks_in, peaks_out, sem.at[1]),
    ]
    for copy in copies:
        copy.start()
    for copy in copies:
        copy.wait()


def kernel(
    R, T, lat_hbm, g1_hbm, w1_hbm, g2_hbm, w2_hbm, up_hbm, dec_ref, peaks_ref,
    lat, g1, g2, rows_in, hist, acc, mix, second, past, w1, w2, up, merged,
    pk1_send, pk1_recv, pk2_send, pk2_recv, pk_second,
    load_sem, x1_send, x1_recv, rl_send, rl_recv, s_send, s_recv, x3_send, x3_recv,
    pk1_ssem, pk1_rsem, pk2_ssem, pk2_rsem, known, spread,
):
    r = lax.axis_index("rows")
    t = lax.axis_index("tm")
    n = R * T
    me = r * T + t
    frames, cols, C = lat.shape
    width = frames * cols

    def there(d):
        return jnp.logical_and(r + d >= 0, r + d < R)

    barrier = pltpu.get_barrier_semaphore()
    near = [(d, e) for d in range(-REACH, REACH + 1) for e in range(T) if (d, e) != (0, 0)]

    def greet(d, e):
        pl.semaphore_signal(
            barrier, inc=1, device_id={"rows": r + d, "tm": lax.rem(t + e, T)}, device_id_type=MESH
        )

    loads = [
        pltpu.make_async_copy(lat_hbm, lat, load_sem.at[0]),
        pltpu.make_async_copy(g1_hbm, g1, load_sem.at[1]),
        pltpu.make_async_copy(g2_hbm, g2, load_sem.at[2]),
        pltpu.make_async_copy(w1_hbm, w1.at[:, 0:C, :], load_sem.at[3]),
        pltpu.make_async_copy(w2_hbm, w2.at[:, 0:C, :], load_sem.at[4]),
        pltpu.make_async_copy(up_hbm, up, load_sem.at[5]),
    ]
    loads[0].start()
    loads[1].start()
    for d, e in near:
        pl.when(there(d))(functools.partial(greet, d, e))
    loads[3].start()
    loads[2].start()

    @pl.when(r == 0)
    def _():
        merged[0] = jnp.zeros_like(merged[0])

    @pl.when(r == R - 1)
    def _():
        merged[2] = jnp.zeros_like(merged[2])

    for d in (-2, -1, 1, 2):

        @pl.when(jnp.logical_not(there(d)))
        def _(d=d):
            rows_in[REACH + d] = jnp.zeros_like(rows_in[REACH + d])
            hist[REACH + d] = jnp.zeros_like(hist[REACH + d])
            if abs(d) == 1:
                second[1 + d] = jnp.zeros_like(second[1 + d])

    pad = w1.shape[1] - C
    w1[:, C:, :] = jnp.zeros((w1.shape[0], pad, C), BF16)
    w2[:, C:, :] = jnp.zeros((w2.shape[0], pad, C), BF16)

    q = lax.broadcasted_iota(jnp.int32, (2 * width, 2 * width), 0)
    o = lax.broadcasted_iota(jnp.int32, (2 * width, 2 * width), 1)
    frame = lax.rem(lax.div(q, cols), frames)
    target = frame * (2 * cols) + 2 * lax.rem(q, cols) + lax.div(q, width)
    spread[...] = jnp.where(o == target, 1.0, 0.0).astype(BF16)

    loads[0].wait()
    loads[1].wait()
    gain1 = g1[...].astype(F32).reshape(1, C)
    own_first = normed_silu(lat[...].astype(F32).reshape(width, C), gain1)
    rows_in[REACH] = packed(own_first, cols)

    rows_near = 1 + jnp.minimum(r, REACH) + jnp.minimum(R - 1 - r, REACH)
    pl.semaphore_wait(barrier, rows_near * T - 1)

    side = 1 - 2 * lax.rem(r, 2)

    def row_copy(d):
        slot = REACH - d
        return pltpu.make_async_remote_copy(
            src_ref=rows_in.at[REACH], dst_ref=rows_in.at[slot], send_sem=x1_send,
            recv_sem=x1_recv.at[slot - jnp.where(slot > REACH, 1, 0)],
            device_id={"rows": r + d}, device_id_type=MESH,
        )

    for d in (side, 2 * side, -2 * side, -side):
        pl.when(there(d))(lambda d=d: row_copy(d).start())

    def relay(slot):
        return pltpu.make_async_remote_copy(
            src_ref=rows_in.at[slot], dst_ref=hist.at[slot], send_sem=rl_send,
            recv_sem=rl_recv.at[slot], device_id={"tm": t + 1}, device_id_type=MESH,
        )

    gives = t < T - 1
    takes = t > 0
    pl.when(gives)(lambda: relay(REACH).start())

    stages = stages_of(R)

    def tell(i):
        for way, d in enumerate((stages[i], -stages[i])):
            pl.when(there(d))(
                lambda way=way, d=d: pl.semaphore_signal(
                    known.at[i, way], inc=1, device_id={"rows": r + d}, device_id_type=MESH
                )
            )

    def hear(i):
        for way, d in enumerate((stages[i], -stages[i])):
            pl.when(there(-d))(lambda way=way: pl.semaphore_wait(known.at[i, way], 1))

    if stages:
        tell(0)

    def two_rows(row):
        rest = jnp.concatenate([row[:, LANES:C], jnp.zeros((1, 2 * LANES - C), F32)], axis=1)
        return jnp.concatenate([row[:, 0:LANES], rest], axis=0)

    pk1_send[...] = two_rows(peak_of(own_first.astype(BF16).astype(F32))).astype(BF16)

    def contribute(source, past_frames):
        f0, f1 = frames_of(source.at[REACH])
        both = jnp.concatenate([f0, f1], axis=0)
        tap = 0 if past_frames else 2
        for at in range(3):
            j = 2 - at
            for k in range(3):
                main = dot(both, w1[(tap * 3 + j) * 3 + k])
                extra = dot(f1 if past_frames else f0, w1[(3 + j) * 3 + k])
                early, late = main[0:cols], main[cols:]
                if past_frames:
                    acc[k, at, 0:cols] += early + extra
                    acc[k, at, cols:] += late
                else:
                    acc[k, at, 0:cols] = early
                    acc[k, at, cols:] = late + extra

    def contribute_side(source, s, past_frames):
        n0, n1 = frames_of(source.at[REACH + s])
        f0, f1 = frames_of(source.at[REACH + 2 * s])
        near_rows = jnp.concatenate([n0, n1], axis=0)
        all_rows = jnp.concatenate([n0, n1, f0, f1], axis=0)
        near_one, far_one = (n1, f1) if past_frames else (n0, f0)
        ones = jnp.concatenate([near_one, far_one], axis=0)
        tap = 0 if past_frames else 2
        mixed = slice(0, cols) if past_frames else slice(cols, width)
        for k in range(3):
            main = dot(all_rows, w1[(tap * 3 + 1 + s) * 3 + k])
            extra = dot(ones, w1[(3 + 1 + s) * 3 + k])
            acc[k, 1] += main[0:width]
            acc[k, 1, mixed] += extra[0:cols]
            acc[k, 1 + s] += main[width:] + dot(near_rows, w1[(tap * 3 + 1) * 3 + k])
            acc[k, 1 + s, mixed] += extra[cols:] + dot(near_one, w1[(3 + 1) * 3 + k])

    loads[3].wait()
    loads[4].start()
    loads[5].start()
    contribute(rows_in, False)

    def await_row(d):
        @pl.when(there(d))
        def _():
            row_copy(-d).wait_recv()
            pl.when(gives)(lambda: relay(REACH + d).start())

    def await_past(d):
        pl.when(there(d))(lambda: relay(REACH + d).wait_recv())

    lane0 = lax.rem(lax.broadcasted_iota(jnp.int32, (width, 1), 0), cols)

    def shifted_sum(left, middle, right):
        left = jnp.where(lane0 == 0, 0.0, pltpu.roll(left, 1, 0))
        right = jnp.where(lane0 == cols - 1, 0.0, pltpu.roll(right, width - 1, 0))
        return left + middle + right

    def activate(o):
        if isinstance(o, int):
            activate_row(o)
        else:
            pl.when(there(o))(lambda: activate_row(o))

    def activate_row(o):
        at = 1 + o
        hidden = shifted_sum(acc[0, at], acc[1, at], acc[2, at]).astype(BF16).astype(F32)
        values = normed_silu(hidden, gain2)
        if isinstance(o, int):
            pk_second[...] = two_rows(peak_of(values.astype(BF16).astype(F32)))
        second[at] = packed(values, cols)

    def hand_on(o):
        at = 1 + o
        return pltpu.make_async_remote_copy(
            src_ref=second.at[at], dst_ref=past.at[at],
            send_sem=s_send, recv_sem=s_recv, device_id={"tm": t + 1}, device_id_type=MESH,
        )

    loads[2].wait()
    gain2 = g2[...].astype(F32).reshape(1, C)

    def handed():
        return pltpu.make_async_remote_copy(
            src_ref=second, dst_ref=past, send_sem=s_send, recv_sem=s_recv,
            device_id={"tm": t + 1}, device_id_type=MESH,
        )

    def second_conv(has_past):
        def frames_at(source):
            pieces = [frames_of(source.at[j]) for j in range(3)]
            return [jnp.concatenate([piece[f] for piece in pieces], axis=1) for f in range(2)]

        def taps_at(i, k):
            return [w2[(i * 3 + j) * 3 + k] for j in range(3)]

        f0, f1 = frames_at(second)
        if has_past:
            handed().wait_recv()
            h0, h1 = frames_at(past)
            early = jnp.concatenate([h0, h1, f0], axis=1)
            late = jnp.concatenate([h1, f0, f1], axis=1)
            lhs = jnp.concatenate([early, late], axis=0)
            for k in range(3):
                taps = [tap for i in range(3) for tap in taps_at(i, k)]
                mix[k] = dot(lhs, jnp.concatenate(taps, axis=0))
        else:
            both = jnp.concatenate([f0, f1], axis=0)
            for k in range(3):
                main = dot(both, jnp.concatenate(taps_at(2, k), axis=0))
                extra = dot(f0, jnp.concatenate(taps_at(1, k), axis=0))
                mix[k, 0:cols] = main[0:cols]
                mix[k, cols:] = main[cols:] + extra

    def meet():
        for i in range(1, len(stages)):
            hear(i - 1)
            tell(i)

    def pass_on(o):
        pl.when(gives)(lambda: hand_on(o).start())

    def peer_of(i):
        p = jnp.where(2 * r >= R, i, n - 2 - i)
        return jnp.where(p >= me, p + 1, p)

    def peak_copy(src, dst, ssem, rsem, peer):
        return pltpu.make_async_remote_copy(
            src_ref=src, dst_ref=dst.at[me - jnp.where(me > peer, 1, 0)], send_sem=ssem, recv_sem=rsem,
            device_id={"rows": peer // T, "tm": lax.rem(peer, T)}, device_id_type=MESH,
        )

    def send_peaks(src, dst, ssem, rsem):
        def step(i, carry):
            peak_copy(src, dst, ssem, rsem, peer_of(i)).start()
            return carry

        lax.fori_loop(0, n - 1, step, 0, unroll=n <= 16)

    def all_peaks(src, dst, ssem, rsem):
        return pltpu.make_async_remote_copy(
            src_ref=dst, dst_ref=dst, send_sem=ssem, recv_sem=rsem,
            device_id={"rows": r, "tm": lax.rem(t + 1, T)}, device_id_type=MESH,
        )

    def take_peaks(*refs):
        src, dst = refs[0:2]
        all_peaks(*refs).wait_recv()

        def step(i, best):
            return jnp.maximum(best, dst[i].astype(F32))

        return lax.fori_loop(0, n - 1, step, src[...].astype(F32), unroll=n <= 16)

    early = (pk1_send, pk1_recv, pk1_ssem, pk1_rsem)
    last = (pk2_send, pk2_recv, pk2_ssem, pk2_rsem)

    def first_peaks():
        if stages:
            hear(len(stages) - 1)
        send_peaks(*early)

    def beside(source, s, past_frames):
        pl.when(there(s))(lambda: contribute_side(source, s, past_frames))

    @pl.when(jnp.logical_not(takes))
    def _():
        await_row(-2)
        meet()
        await_row(side)
        await_row(2)
        beside(rows_in, side, False)
        activate(side)
        pass_on(side)
        await_row(-side)
        beside(rows_in, -side, False)
        activate(0)
        pass_on(0)
        activate(-side)
        pass_on(-side)
        first_peaks()
        loads[4].wait()
        second_conv(False)

    @pl.when(takes)
    def _():
        relay(REACH).wait_recv()
        contribute(hist, True)
        meet()
        await_row(-2)
        await_row(side)
        await_row(2)
        beside(rows_in, side, False)
        await_row(-side)
        beside(rows_in, -side, False)
        loads[4].wait()
        first_peaks()
        await_past(-2)
        await_past(side)
        await_past(2)
        beside(hist, side, True)
        await_past(-side)
        beside(hist, -side, True)
        activate(side)
        activate(0)
        activate(-side)
        second_conv(True)

    block = lat[...].astype(F32).reshape(width, C) + shifted_sum(mix[0], mix[1], mix[2])
    block = block.astype(BF16)
    wide_block = block.astype(F32)
    merged[1] = packed(wide_block, cols)
    pk2_send[...] = jnp.concatenate([pk_second[...], two_rows(peak_of(wide_block))], axis=0).astype(BF16)
    send_peaks(*last)

    def edge_copy(d):
        slot = 1 - d
        return pltpu.make_async_remote_copy(
            src_ref=merged.at[1], dst_ref=merged.at[slot], send_sem=x3_send,
            recv_sem=x3_recv.at[slot // 2], device_id={"rows": r + d}, device_id_type=MESH,
        )

    for d in (side, -side):
        pl.when(there(d))(lambda d=d: edge_copy(d).start())

    loads[5].wait()
    C2 = dec_ref.shape[2]
    own = dot_nt(up[...], block).reshape(3, 3, C2, width)
    upper = own[1] + own[2]
    lower = own[0] + own[1]

    def edge_row(slot):
        f0, f1 = frames_of(merged.at[slot])
        return jnp.concatenate([f0, f1], axis=0)[:, 0:C]

    for d in (side, -side):
        pl.when(there(d))(lambda d=d: edge_copy(-d).wait_recv())
    upper = upper + dot_nt(up[0 : 3 * C2], edge_row(0)).reshape(3, C2, width)
    lower = lower + dot_nt(up[6 * C2 :], edge_row(2)).reshape(3, C2, width)
    lane = lax.rem(lax.broadcasted_iota(jnp.int32, (C2, width), 1), cols)

    def columns(sums):
        from_left = jnp.where(lane == 0, 0.0, pltpu.roll(sums[0], 1, 1))
        from_right = jnp.where(lane == cols - 1, 0.0, pltpu.roll(sums[2], width - 1, 1))
        even = from_left + sums[1] + sums[2]
        odd = sums[0] + sums[1] + from_right
        return jnp.concatenate([even, odd], axis=1).astype(BF16)

    narrow = jnp.concatenate([columns(upper), columns(lower)], axis=0)
    wide = dot(narrow, spread[...]).astype(BF16)
    for f in range(frames):
        for j in range(2):
            dec_ref[f, j] = wide[j * C2 : (j + 1) * C2, f * 2 * cols : (f + 1) * 2 * cols]

    best = jnp.concatenate([take_peaks(*early), take_peaks(*last)], axis=0)
    for i in range(3):
        peaks_ref[i : i + 1, 0:LANES] = best[2 * i : 2 * i + 1, :]
        peaks_ref[i : i + 1, LANES:C] = best[2 * i + 1 : 2 * i + 2, 0 : C - LANES]

    all_peaks(*early).wait_send()
    all_peaks(*last).wait_send()

    def sent(ref, sem, count, most):
        for c in range(1, most + 1):
            pl.when(count == c)(
                lambda c=c: pltpu.make_async_remote_copy(
                    src_ref=ref.at[pl.ds(0, c)], dst_ref=ref.at[pl.ds(0, c)], send_sem=sem, recv_sem=sem,
                    device_id={"rows": r, "tm": lax.rem(t + 1, T)}, device_id_type=MESH,
                ).wait_send()
            )

    sent(rows_in, x1_send, rows_near - 1, 2 * REACH)
    sent(merged, x3_send, jnp.minimum(r, 1) + jnp.minimum(R - 1 - r, 1), 2)

    @pl.when(gives)
    def _():
        sent(rows_in, rl_send, rows_near, 2 * REACH + 1)
        handed().wait_send()


def per_device(latent, gain_first, conv_first, gain_second, conv_second, conv_up):
    frames, rows, cols, C = latent.shape
    R, T = lax.axis_size("rows"), lax.axis_size("tm")
    C2 = conv_up.shape[2]
    n = R * T
    if rows != 1 or frames != 2 or 2 * C != 3 * LANES:
        raise ValueError("unsupported block")
    depth = 2 * LANES
    taps = conv_first.shape[0] * conv_first.shape[1] * conv_first.shape[2]
    vmem = pl.BlockSpec(memory_space=pltpu.VMEM)
    hbm = pl.BlockSpec(memory_space=pltpu.HBM)
    dma = pltpu.SemaphoreType.DMA
    span = 2 * REACH + 1
    width = frames * cols
    decoded, peaks = pl.pallas_call(
        functools.partial(kernel, R, T),
        out_shape=(
            pltpu.VMEM((frames, 2 * rows, C2, 2 * cols), BF16),
            pltpu.VMEM((3, C), F32),
        ),
        in_specs=[hbm] * 6,
        out_specs=(vmem, vmem),
        scratch_shapes=[
            pltpu.VMEM((frames, cols, C), BF16),
            pltpu.VMEM((C,), BF16),
            pltpu.VMEM((C,), BF16),
            pltpu.VMEM((span, 3, cols, LANES), BF16),
            pltpu.VMEM((span, 3, cols, LANES), BF16),
            pltpu.VMEM((3, 3, width, C), F32),
            pltpu.VMEM((3, width, C), F32),
            pltpu.VMEM((3, 3, cols, LANES), BF16),
            pltpu.VMEM((3, 3, cols, LANES), BF16),
            pltpu.VMEM((taps, depth, C), BF16),
            pltpu.VMEM((taps, depth, C), BF16),
            pltpu.VMEM((9 * C2, C), BF16),
            pltpu.VMEM((3, 3, cols, LANES), BF16),
            pltpu.VMEM((2, LANES), BF16),
            pltpu.VMEM((n - 1, 2, LANES), BF16),
            pltpu.VMEM((4, LANES), BF16),
            pltpu.VMEM((n - 1, 4, LANES), BF16),
            pltpu.VMEM((2, LANES), F32),
            dma((6,)),
            dma,
            dma((span - 1,)),
            dma,
            dma((span,)),
            dma,
            dma,
            dma,
            dma((2,)),
            dma,
            dma,
            dma,
            dma,
            pltpu.SemaphoreType.REGULAR((max(1, len(stages_of(R))), 2)),
            pltpu.VMEM((2 * width, 2 * width), BF16),
        ],
        compiler_params=pltpu.CompilerParams(collective_id=0, has_side_effects=True, vmem_limit_bytes=54 * 2**20),
    )(
        latent.reshape(frames, cols, C),
        gain_first,
        conv_first.reshape(taps, C, C),
        gain_second,
        conv_second.reshape(taps, C, C),
        conv_up.reshape(9 * C2, C),
    )
    return pl.pallas_call(
        finish,
        out_shape=(
            jax.ShapeDtypeStruct(decoded.shape, BF16),
            jax.ShapeDtypeStruct(peaks.shape, F32),
        ),
        in_specs=[vmem, vmem],
        out_specs=(hbm, hbm),
        scratch_shapes=[dma((2,))],
        compiler_params=pltpu.CompilerParams(vmem_limit_bytes=2**20),
    )(decoded, peaks)


def solution(mesh):
    return jax.shard_map(
        per_device,
        mesh=mesh,
        in_specs=(P(("clip", "tm"), "rows", None, None), P(), P(), P(), P(), P()),
        out_specs=(P(("clip", "tm"), "rows", None, None), P("clip", None)),
        check_vma=False,
    )
```

```python
import functools

import jax
import jax.numpy as jnp
from jax import lax
from jax.experimental import pallas as pl
from jax.experimental.pallas import tpu as pltpu
from jax.sharding import PartitionSpec as P

MESH = pl.DeviceIdType.MESH
BF16 = jnp.bfloat16
F32 = jnp.float32
REACH = 2
LANES = 128


def stages_of(R):
    return [REACH << i for i in range(R.bit_length()) if (REACH << i) < R - 1]


def normed_silu(values, gain):
    scale = lax.rsqrt(jnp.mean(values * values, axis=-1, keepdims=True) + 1e-06)
    u = values * scale * gain
    return u / (1.0 + jnp.exp(-u))


def peak_of(values):
    return jnp.max(jnp.abs(values), axis=0, keepdims=True)


def dot(a, b):
    return jnp.dot(a, b, preferred_element_type=F32)


def dot_nt(a, b):
    return lax.dot_general(a, b, (((1,), (1,)), ((), ())), preferred_element_type=F32)


def packed(values, cols):
    low = values[:, 0:LANES].reshape(2, cols, LANES)
    high = jnp.concatenate([values[0:cols, LANES:], values[cols:, LANES:]], axis=1)
    return jnp.concatenate([low, high[None]], axis=0).astype(BF16)


def frames_of(buf):
    high = buf[2]
    turned = pltpu.roll(high.astype(F32), LANES // 2, 1).astype(BF16)
    return jnp.concatenate([buf[0], high], axis=1), jnp.concatenate([buf[1], turned], axis=1)


def finish(dec_in, peaks_in, dec_out, peaks_out, sem):
    copies = [
        pltpu.make_async_copy(dec_in, dec_out, sem.at[0]),
        pltpu.make_async_copy(peaks_in, peaks_out, sem.at[1]),
    ]
    for copy in copies:
        copy.start()
    for copy in copies:
        copy.wait()


def kernel(
    R, T, lat_hbm, g1_hbm, w1_hbm, g2_hbm, w2_hbm, up_hbm, dec_ref, peaks_ref,
    lat, g1, g2, rows_in, hist, acc, mix, gift, gift_out, base, second, w1, w2, up, merged,
    pk_send, pk_recv, pk_first, pk_second,
    load_sem, x1_send, x1_recv, rl_send, rl_recv, s_send, s_recv, x3_send, x3_recv,
    pk_ssem, pk_rsem, known, spread,
):
    r = lax.axis_index("rows")
    t = lax.axis_index("tm")
    n = R * T
    me = r * T + t
    frames, cols, C = lat.shape
    width = frames * cols

    def there(d):
        return jnp.logical_and(r + d >= 0, r + d < R)

    barrier = pltpu.get_barrier_semaphore()
    near = [(d, e) for d in range(-REACH, REACH + 1) for e in range(T) if (d, e) != (0, 0)]

    def greet(d, e):
        pl.semaphore_signal(
            barrier, inc=1, device_id={"rows": r + d, "tm": lax.rem(t + e, T)}, device_id_type=MESH
        )

    loads = [
        pltpu.make_async_copy(lat_hbm, lat, load_sem.at[0]),
        pltpu.make_async_copy(g1_hbm, g1, load_sem.at[1]),
        pltpu.make_async_copy(g2_hbm, g2, load_sem.at[2]),
        pltpu.make_async_copy(w1_hbm, w1.at[:, 0:C, :], load_sem.at[3]),
        pltpu.make_async_copy(w2_hbm, w2.at[:, 0:C, :], load_sem.at[4]),
        pltpu.make_async_copy(up_hbm, up, load_sem.at[5]),
    ]
    loads[0].start()
    loads[1].start()
    for d, e in near:
        pl.when(there(d))(functools.partial(greet, d, e))
    loads[3].start()
    loads[2].start()

    @pl.when(r == 0)
    def _():
        merged[0] = jnp.zeros_like(merged[0])

    @pl.when(r == R - 1)
    def _():
        merged[2] = jnp.zeros_like(merged[2])

    for d in (-2, -1, 1, 2):

        @pl.when(jnp.logical_not(there(d)))
        def _(d=d):
            rows_in[REACH + d] = jnp.zeros_like(rows_in[REACH + d])
            hist[REACH + d] = jnp.zeros_like(hist[REACH + d])

    second[...] = jnp.zeros_like(second)

    @pl.when(t == 0)
    def _():
        gift[...] = jnp.zeros_like(gift)

    pad = w1.shape[1] - C
    w1[:, C:, :] = jnp.zeros((w1.shape[0], pad, C), BF16)
    w2[:, C:, :] = jnp.zeros((w2.shape[0], pad, C), BF16)

    q = lax.broadcasted_iota(jnp.int32, (2 * width, 2 * width), 0)
    o = lax.broadcasted_iota(jnp.int32, (2 * width, 2 * width), 1)
    frame = lax.rem(lax.div(q, cols), frames)
    target = frame * (2 * cols) + 2 * lax.rem(q, cols) + lax.div(q, width)
    spread[...] = jnp.where(o == target, 1.0, 0.0).astype(BF16)

    loads[0].wait()
    loads[1].wait()
    gain1 = g1[...].astype(F32).reshape(1, C)
    own_first = normed_silu(lat[...].astype(F32).reshape(width, C), gain1)
    rows_in[REACH] = packed(own_first, cols)

    rows_near = 1 + jnp.minimum(r, REACH) + jnp.minimum(R - 1 - r, REACH)
    pl.semaphore_wait(barrier, rows_near * T - 1)

    side = 1 - 2 * lax.rem(r, 2)

    def row_copy(d):
        slot = REACH - d
        return pltpu.make_async_remote_copy(
            src_ref=rows_in.at[REACH], dst_ref=rows_in.at[slot], send_sem=x1_send,
            recv_sem=x1_recv.at[slot - jnp.where(slot > REACH, 1, 0)],
            device_id={"rows": r + d}, device_id_type=MESH,
        )

    for d in (side, 2 * side, -2 * side, -side):
        pl.when(there(d))(lambda d=d: row_copy(d).start())

    def relay(slot):
        return pltpu.make_async_remote_copy(
            src_ref=rows_in.at[slot], dst_ref=hist.at[slot], send_sem=rl_send,
            recv_sem=rl_recv.at[slot], device_id={"tm": t + 1}, device_id_type=MESH,
        )

    gives = t < T - 1
    takes = t > 0
    pl.when(gives)(lambda: relay(REACH).start())

    stages = stages_of(R)

    def tell(i):
        for way, d in enumerate((stages[i], -stages[i])):
            pl.when(there(d))(
                lambda way=way, d=d: pl.semaphore_signal(
                    known.at[i, way], inc=1, device_id={"rows": r + d}, device_id_type=MESH
                )
            )

    def hear(i):
        for way, d in enumerate((stages[i], -stages[i])):
            pl.when(there(-d))(lambda way=way: pl.semaphore_wait(known.at[i, way], 1))

    if stages:
        tell(0)

    def two_rows(row):
        rest = jnp.concatenate([row[:, LANES:C], jnp.zeros((1, 2 * LANES - C), F32)], axis=1)
        return jnp.concatenate([row[:, 0:LANES], rest], axis=0)

    pk_first[...] = two_rows(peak_of(own_first.astype(BF16).astype(F32)))

    def contribute(source, past_frames):
        f0, f1 = frames_of(source.at[REACH])
        both = jnp.concatenate([f0, f1], axis=0)
        tap = 0 if past_frames else 2
        for at in range(3):
            j = 2 - at
            for k in range(3):
                main = dot(both, w1[(tap * 3 + j) * 3 + k])
                extra = dot(f1 if past_frames else f0, w1[(3 + j) * 3 + k])
                early, late = main[0:cols], main[cols:]
                if past_frames:
                    acc[k, at, 0:cols] += early + extra
                    acc[k, at, cols:] += late
                else:
                    acc[k, at, 0:cols] = early
                    acc[k, at, cols:] = late + extra

    def contribute_side(source, s, past_frames):
        n0, n1 = frames_of(source.at[REACH + s])
        f0, f1 = frames_of(source.at[REACH + 2 * s])
        near_rows = jnp.concatenate([n0, n1], axis=0)
        all_rows = jnp.concatenate([n0, n1, f0, f1], axis=0)
        near_one, far_one = (n1, f1) if past_frames else (n0, f0)
        ones = jnp.concatenate([near_one, far_one], axis=0)
        tap = 0 if past_frames else 2
        mixed = slice(0, cols) if past_frames else slice(cols, width)
        for k in range(3):
            main = dot(all_rows, w1[(tap * 3 + 1 + s) * 3 + k])
            extra = dot(ones, w1[(3 + 1 + s) * 3 + k])
            acc[k, 1] += main[0:width]
            acc[k, 1, mixed] += extra[0:cols]
            acc[k, 1 + s] += main[width:] + dot(near_rows, w1[(tap * 3 + 1) * 3 + k])
            acc[k, 1 + s, mixed] += extra[cols:] + dot(near_one, w1[(3 + 1) * 3 + k])

    loads[3].wait()
    loads[4].start()
    loads[5].start()
    contribute(rows_in, False)

    def await_row(d):
        @pl.when(there(d))
        def _():
            row_copy(-d).wait_recv()
            pl.when(gives)(lambda: relay(REACH + d).start())

    def await_past(d):
        pl.when(there(d))(lambda: relay(REACH + d).wait_recv())

    lane0 = lax.rem(lax.broadcasted_iota(jnp.int32, (width, 1), 0), cols)

    def shifted_sum(left, middle, right):
        left = jnp.where(lane0 == 0, 0.0, pltpu.roll(left, 1, 0))
        right = jnp.where(lane0 == cols - 1, 0.0, pltpu.roll(right, width - 1, 0))
        return left + middle + right

    def activate(slot):
        o = (side, 0, -side)[slot]
        if slot == 1:
            activate_row(slot, o)
        else:
            pl.when(there(o))(lambda: activate_row(slot, o))

    def activate_row(slot, o):
        at = 1 + o
        hidden = shifted_sum(acc[0, at], acc[1, at], acc[2, at]).astype(BF16).astype(F32)
        values = normed_silu(hidden, gain2).astype(BF16)
        if slot == 1:
            pk_second[...] = two_rows(peak_of(values.astype(F32)))
        second[slot, :, 0:C] = values

    def gift_copy():
        return pltpu.make_async_remote_copy(
            src_ref=gift_out, dst_ref=gift, send_sem=s_send, recv_sem=s_recv,
            device_id={"tm": t + 1}, device_id_type=MESH,
        )

    loads[2].wait()
    gain2 = g2[...].astype(F32).reshape(1, C)

    def second_conv(past_frames):
        rows = [second[slot] for slot in range(3)]
        both = jnp.concatenate(rows, axis=1)
        one = jnp.concatenate([row[cols:] if past_frames else row[0:cols] for row in rows], axis=1)

        def taps_at(i, k):
            return jnp.concatenate([w2[(i * 3 + 1 + o) * 3 + k] for o in (side, 0, -side)], axis=0)

        sums = []
        for k in range(3):
            main = dot(both, taps_at(0 if past_frames else 2, k))
            extra = dot(one, taps_at(1, k))
            if past_frames:
                sums.append(jnp.concatenate([main[0:cols] + extra, main[cols:]], axis=0))
            else:
                sums.append(jnp.concatenate([main[0:cols], main[cols:] + extra], axis=0))
        if past_frames:
            gift_out[...] = shifted_sum(*sums).astype(BF16)
        else:
            mix[...] = shifted_sum(*sums)

    def meet():
        for i in range(1, len(stages)):
            hear(i - 1)
            tell(i)

    def peak_copy(peer):
        return pltpu.make_async_remote_copy(
            src_ref=pk_send, dst_ref=pk_recv.at[me - jnp.where(me > peer, 1, 0)],
            send_sem=pk_ssem, recv_sem=pk_rsem,
            device_id={"rows": peer // T, "tm": lax.rem(peer, T)}, device_id_type=MESH,
        )

    def send_peaks():
        def step(i, carry):
            p = jnp.where(2 * r >= R, i, n - 2 - i)
            peak_copy(jnp.where(p >= me, p + 1, p)).start()
            return carry

        lax.fori_loop(0, n - 1, step, 0, unroll=n <= 16)

    def all_peaks():
        return pltpu.make_async_remote_copy(
            src_ref=pk_recv, dst_ref=pk_recv, send_sem=pk_ssem, recv_sem=pk_rsem,
            device_id={"rows": r, "tm": lax.rem(t + 1, T)}, device_id_type=MESH,
        )

    def heard():
        if stages:
            hear(len(stages) - 1)

    def beside(source, s, past_frames):
        pl.when(there(s))(lambda: contribute_side(source, s, past_frames))

    @pl.when(jnp.logical_not(takes))
    def _():
        await_row(-2)
        meet()
        await_row(side)
        await_row(2)
        beside(rows_in, side, False)
        await_row(-side)
        activate(0)
        beside(rows_in, -side, False)
        activate(1)
        activate(2)
        loads[4].wait()

        @pl.when(gives)
        def _():
            second_conv(True)
            gift_copy().start()

        second_conv(False)

    @pl.when(takes)
    def _():
        relay(REACH).wait_recv()
        contribute(hist, True)
        meet()
        await_row(-2)
        await_row(side)
        await_row(2)
        beside(rows_in, side, False)
        await_row(-side)
        beside(rows_in, -side, False)
        loads[4].wait()
        heard()
        await_past(-2)
        await_past(side)
        await_past(2)
        beside(hist, side, True)
        activate(0)
        await_past(-side)
        beside(hist, -side, True)
        activate(1)
        activate(2)
        second_conv(False)
        gift_copy().wait_recv()

    block = lat[...].astype(F32).reshape(width, C) + mix[...] + gift[...].astype(F32)
    block = block.astype(BF16)
    wide_block = block.astype(F32)
    merged[1] = packed(wide_block, cols)
    peaks = jnp.concatenate([pk_first[...], pk_second[...], two_rows(peak_of(wide_block))], axis=0)
    pk_send[...] = peaks.astype(BF16)
    pl.when(jnp.logical_not(takes))(heard)
    send_peaks()

    def edge_copy(d):
        slot = 1 - d
        return pltpu.make_async_remote_copy(
            src_ref=merged.at[1], dst_ref=merged.at[slot], send_sem=x3_send,
            recv_sem=x3_recv.at[slot // 2], device_id={"rows": r + d}, device_id_type=MESH,
        )

    for d in (side, -side):
        pl.when(there(d))(lambda d=d: edge_copy(d).start())

    loads[5].wait()
    C2 = dec_ref.shape[2]
    own = dot_nt(up[...], block).reshape(3, 3, C2, width)
    base[0] = own[1] + own[2]
    base[1] = own[0] + own[1]
    lane = lax.rem(lax.broadcasted_iota(jnp.int32, (C2, width), 1), cols)

    def columns(sums):
        from_left = jnp.where(lane == 0, 0.0, pltpu.roll(sums[0], 1, 1))
        from_right = jnp.where(lane == cols - 1, 0.0, pltpu.roll(sums[2], width - 1, 1))
        even = from_left + sums[1] + sums[2]
        odd = sums[0] + sums[1] + from_right
        return jnp.concatenate([even, odd], axis=1).astype(BF16)

    def decode_row(half):
        f0, f1 = frames_of(merged.at[2 * half])
        rows = jnp.concatenate([f0, f1], axis=0)[:, 0:C]
        taps = up[half * 6 * C2 : (half * 6 + 3) * C2]
        sums = base[half] + dot_nt(taps, rows).reshape(3, C2, width)
        wide = dot(columns(sums), spread[...]).astype(BF16)
        for f in range(frames):
            dec_ref[f, half] = wide[:, f * 2 * cols : (f + 1) * 2 * cols]

    for d in (-1, 1):
        pl.when(there(d))(lambda d=d: edge_copy(-d).wait_recv())
        decode_row((1 + d) // 2)

    all_peaks().wait_recv()

    def take_peak(i, best):
        return jnp.maximum(best, pk_recv[i].astype(F32))

    best = lax.fori_loop(0, n - 1, take_peak, peaks, unroll=n <= 16)
    for i in range(3):
        peaks_ref[i : i + 1, 0:LANES] = best[2 * i : 2 * i + 1, :]
        peaks_ref[i : i + 1, LANES:C] = best[2 * i + 1 : 2 * i + 2, 0 : C - LANES]

    def sent(ref, sem, count, most):
        for c in range(1, most + 1):
            pl.when(count == c)(
                lambda c=c: pltpu.make_async_remote_copy(
                    src_ref=ref.at[pl.ds(0, c)], dst_ref=ref.at[pl.ds(0, c)], send_sem=sem, recv_sem=sem,
                    device_id={"rows": r, "tm": lax.rem(t + 1, T)}, device_id_type=MESH,
                ).wait_send()
            )

    sent(rows_in, x1_send, rows_near - 1, 2 * REACH)
    sent(merged, x3_send, jnp.minimum(r, 1) + jnp.minimum(R - 1 - r, 1), 2)

    @pl.when(gives)
    def _():
        sent(rows_in, rl_send, rows_near, 2 * REACH + 1)
        gift_copy().wait_send()

    all_peaks().wait_send()


def per_device(latent, gain_first, conv_first, gain_second, conv_second, conv_up):
    frames, rows, cols, C = latent.shape
    R, T = lax.axis_size("rows"), lax.axis_size("tm")
    C2 = conv_up.shape[2]
    n = R * T
    if rows != 1 or frames != 2 or 2 * C != 3 * LANES:
        raise ValueError("unsupported block")
    depth = 2 * LANES
    taps = conv_first.shape[0] * conv_first.shape[1] * conv_first.shape[2]
    vmem = pl.BlockSpec(memory_space=pltpu.VMEM)
    hbm = pl.BlockSpec(memory_space=pltpu.HBM)
    dma = pltpu.SemaphoreType.DMA
    span = 2 * REACH + 1
    width = frames * cols
    decoded, peaks = pl.pallas_call(
        functools.partial(kernel, R, T),
        out_shape=(
            pltpu.VMEM((frames, 2 * rows, C2, 2 * cols), BF16),
            pltpu.VMEM((3, C), F32),
        ),
        in_specs=[hbm] * 6,
        out_specs=(vmem, vmem),
        scratch_shapes=[
            pltpu.VMEM((frames, cols, C), BF16),
            pltpu.VMEM((C,), BF16),
            pltpu.VMEM((C,), BF16),
            pltpu.VMEM((span, 3, cols, LANES), BF16),
            pltpu.VMEM((span, 3, cols, LANES), BF16),
            pltpu.VMEM((3, 3, width, C), F32),
            pltpu.VMEM((width, C), F32),
            pltpu.VMEM((width, C), BF16),
            pltpu.VMEM((width, C), BF16),
            pltpu.VMEM((2, 3, C2, width), F32),
            pltpu.VMEM((3, width, depth), BF16),
            pltpu.VMEM((taps, depth, C), BF16),
            pltpu.VMEM((taps, depth, C), BF16),
            pltpu.VMEM((9 * C2, C), BF16),
            pltpu.VMEM((3, 3, cols, LANES), BF16),
            pltpu.VMEM((6, LANES), BF16),
            pltpu.VMEM((n - 1, 6, LANES), BF16),
            pltpu.VMEM((2, LANES), F32),
            pltpu.VMEM((2, LANES), F32),
            dma((6,)),
            dma,
            dma((span - 1,)),
            dma,
            dma((span,)),
            dma,
            dma,
            dma,
            dma((2,)),
            dma,
            dma,
            pltpu.SemaphoreType.REGULAR((max(1, len(stages_of(R))), 2)),
            pltpu.VMEM((2 * width, 2 * width), BF16),
        ],
        compiler_params=pltpu.CompilerParams(collective_id=0, has_side_effects=True, vmem_limit_bytes=54 * 2**20),
    )(
        latent.reshape(frames, cols, C),
        gain_first,
        conv_first.reshape(taps, C, C),
        gain_second,
        conv_second.reshape(taps, C, C),
        conv_up.reshape(9 * C2, C),
    )
    return pl.pallas_call(
        finish,
        out_shape=(
            jax.ShapeDtypeStruct(decoded.shape, BF16),
            jax.ShapeDtypeStruct(peaks.shape, F32),
        ),
        in_specs=[vmem, vmem],
        out_specs=(hbm, hbm),
        scratch_shapes=[dma((2,))],
        compiler_params=pltpu.CompilerParams(vmem_limit_bytes=2**20),
    )(decoded, peaks)


def solution(mesh):
    return jax.shard_map(
        per_device,
        mesh=mesh,
        in_specs=(P(("clip", "tm"), "rows", None, None), P(), P(), P(), P(), P()),
        out_specs=(P(("clip", "tm"), "rows", None, None), P("clip", None)),
        check_vma=False,
    )
```

```python
import functools

import jax
import jax.numpy as jnp
from jax import lax
from jax.experimental import pallas as pl
from jax.experimental.pallas import tpu as pltpu
from jax.sharding import PartitionSpec as P

MESH = pl.DeviceIdType.MESH
BF16 = jnp.bfloat16
F32 = jnp.float32
REACH = 2
LANES = 128


def stages_of(R):
    return [REACH << i for i in range(R.bit_length()) if (REACH << i) < R - 1]


def normed_silu(values, gain):
    scale = lax.rsqrt(jnp.mean(values * values, axis=-1, keepdims=True) + 1e-06)
    u = values * scale * gain
    return u / (1.0 + jnp.exp(-u))


def peak_of(values):
    return jnp.max(jnp.abs(values), axis=0, keepdims=True)


def dot(a, b):
    return jnp.dot(a, b, preferred_element_type=F32)


def dot_nt(a, b):
    return lax.dot_general(a, b, (((1,), (1,)), ((), ())), preferred_element_type=F32)


def packed(values, cols):
    low = values[:, 0:LANES].reshape(2, cols, LANES)
    high = jnp.concatenate([values[0:cols, LANES:], values[cols:, LANES:]], axis=1)
    return jnp.concatenate([low, high[None]], axis=0).astype(BF16)


def frames_of(buf):
    high = buf[2]
    turned = pltpu.roll(high.astype(F32), LANES // 2, 1).astype(BF16)
    return jnp.concatenate([buf[0], high], axis=1), jnp.concatenate([buf[1], turned], axis=1)


def finish(dec_in, peaks_in, dec_out, peaks_out, sem):
    copies = [
        pltpu.make_async_copy(dec_in, dec_out, sem.at[0]),
        pltpu.make_async_copy(peaks_in, peaks_out, sem.at[1]),
    ]
    for copy in copies:
        copy.start()
    for copy in copies:
        copy.wait()


def kernel(
    R, T, lat_hbm, g1_hbm, w1_hbm, g2_hbm, w2_hbm, up_hbm, dec_ref, peaks_ref,
    lat, g1, g2, rows_in, hist, acc, mix, gift, gift_out, base, second, w1, w2, up, merged,
    pk_send, pk_recv, pk_past, pk_first, pk_second,
    load_sem, x1_send, x1_recv, rl_send, rl_recv, s_send, s_recv, x3_send, x3_recv,
    pk_ssem, pk_rsem, pp_rsem, known, spread,
):
    r = lax.axis_index("rows")
    t = lax.axis_index("tm")
    n = R * T
    me = r * T + t
    frames, cols, C = lat.shape
    width = frames * cols

    def there(d):
        return jnp.logical_and(r + d >= 0, r + d < R)

    barrier = pltpu.get_barrier_semaphore()
    near = [(d, e) for d in range(-REACH, REACH + 1) for e in range(T) if (d, e) != (0, 0)]

    def greet(d, e):
        pl.semaphore_signal(
            barrier, inc=1, device_id={"rows": r + d, "tm": lax.rem(t + e, T)}, device_id_type=MESH
        )

    loads = [
        pltpu.make_async_copy(lat_hbm, lat, load_sem.at[0]),
        pltpu.make_async_copy(g1_hbm, g1, load_sem.at[1]),
        pltpu.make_async_copy(g2_hbm, g2, load_sem.at[2]),
        pltpu.make_async_copy(w1_hbm, w1.at[:, 0:C, :], load_sem.at[3]),
        pltpu.make_async_copy(w2_hbm, w2.at[:, 0:C, :], load_sem.at[4]),
        pltpu.make_async_copy(up_hbm, up, load_sem.at[5]),
    ]
    loads[0].start()
    loads[1].start()
    for d, e in near:
        pl.when(there(d))(functools.partial(greet, d, e))
    loads[3].start()
    loads[2].start()

    @pl.when(r == 0)
    def _():
        merged[0] = jnp.zeros_like(merged[0])

    @pl.when(r == R - 1)
    def _():
        merged[2] = jnp.zeros_like(merged[2])

    for d in (-2, -1, 1, 2):

        @pl.when(jnp.logical_not(there(d)))
        def _(d=d):
            rows_in[REACH + d] = jnp.zeros_like(rows_in[REACH + d])
            hist[REACH + d] = jnp.zeros_like(hist[REACH + d])

    second[...] = jnp.zeros_like(second)

    @pl.when(t == 0)
    def _():
        gift[...] = jnp.zeros_like(gift)

    pad = w1.shape[1] - C
    w1[:, C:, :] = jnp.zeros((w1.shape[0], pad, C), BF16)
    w2[:, C:, :] = jnp.zeros((w2.shape[0], pad, C), BF16)

    q = lax.broadcasted_iota(jnp.int32, (2 * width, 2 * width), 0)
    o = lax.broadcasted_iota(jnp.int32, (2 * width, 2 * width), 1)
    frame = lax.rem(lax.div(q, cols), frames)
    target = frame * (2 * cols) + 2 * lax.rem(q, cols) + lax.div(q, width)
    spread[...] = jnp.where(o == target, 1.0, 0.0).astype(BF16)

    loads[0].wait()
    loads[1].wait()
    gain1 = g1[...].astype(F32).reshape(1, C)
    own_first = normed_silu(lat[...].astype(F32).reshape(width, C), gain1)
    rows_in[REACH] = packed(own_first, cols)

    rows_near = 1 + jnp.minimum(r, REACH) + jnp.minimum(R - 1 - r, REACH)
    pl.semaphore_wait(barrier, rows_near * T - 1)

    side = 1 - 2 * lax.rem(r, 2)

    def row_copy(d):
        slot = REACH - d
        return pltpu.make_async_remote_copy(
            src_ref=rows_in.at[REACH], dst_ref=rows_in.at[slot], send_sem=x1_send,
            recv_sem=x1_recv.at[slot - jnp.where(slot > REACH, 1, 0)],
            device_id={"rows": r + d}, device_id_type=MESH,
        )

    for d in (side, 2 * side, -2 * side, -side):
        pl.when(there(d))(lambda d=d: row_copy(d).start())

    def relay(slot):
        return pltpu.make_async_remote_copy(
            src_ref=rows_in.at[slot], dst_ref=hist.at[slot], send_sem=rl_send,
            recv_sem=rl_recv.at[slot], device_id={"tm": t + 1}, device_id_type=MESH,
        )

    gives = t < T - 1
    takes = t > 0
    pl.when(gives)(lambda: relay(REACH).start())

    stages = stages_of(R)

    def tell(i):
        for way, d in enumerate((stages[i], -stages[i])):
            pl.when(there(d))(
                lambda way=way, d=d: pl.semaphore_signal(
                    known.at[i, way], inc=1, device_id={"rows": r + d}, device_id_type=MESH
                )
            )

    def hear(i):
        for way, d in enumerate((stages[i], -stages[i])):
            pl.when(there(-d))(lambda way=way: pl.semaphore_wait(known.at[i, way], 1))

    if stages:
        tell(0)

    def two_rows(row):
        rest = jnp.concatenate([row[:, LANES:C], jnp.zeros((1, 2 * LANES - C), F32)], axis=1)
        return jnp.concatenate([row[:, 0:LANES], rest], axis=0)

    pk_first[...] = two_rows(peak_of(own_first.astype(BF16).astype(F32)))

    def contribute(source, past_frames):
        f0, f1 = frames_of(source.at[REACH])
        both = jnp.concatenate([f0, f1], axis=0)
        tap = 0 if past_frames else 2
        for at in range(3):
            j = 2 - at
            for k in range(3):
                main = dot(both, w1[(tap * 3 + j) * 3 + k])
                extra = dot(f1 if past_frames else f0, w1[(3 + j) * 3 + k])
                early, late = main[0:cols], main[cols:]
                if past_frames:
                    acc[k, at, 0:cols] += early + extra
                    acc[k, at, cols:] += late
                else:
                    acc[k, at, 0:cols] = early
                    acc[k, at, cols:] = late + extra

    def contribute_side(source, s, past_frames):
        n0, n1 = frames_of(source.at[REACH + s])
        f0, f1 = frames_of(source.at[REACH + 2 * s])
        near_rows = jnp.concatenate([n0, n1], axis=0)
        all_rows = jnp.concatenate([n0, n1, f0, f1], axis=0)
        near_one, far_one = (n1, f1) if past_frames else (n0, f0)
        ones = jnp.concatenate([near_one, far_one], axis=0)
        tap = 0 if past_frames else 2
        mixed = slice(0, cols) if past_frames else slice(cols, width)
        for k in range(3):
            main = dot(all_rows, w1[(tap * 3 + 1 + s) * 3 + k])
            extra = dot(ones, w1[(3 + 1 + s) * 3 + k])
            acc[k, 1] += main[0:width]
            acc[k, 1, mixed] += extra[0:cols]
            acc[k, 1 + s] += main[width:] + dot(near_rows, w1[(tap * 3 + 1) * 3 + k])
            acc[k, 1 + s, mixed] += extra[cols:] + dot(near_one, w1[(3 + 1) * 3 + k])

    loads[3].wait()
    loads[4].start()
    loads[5].start()
    contribute(rows_in, False)

    def await_row(d):
        @pl.when(there(d))
        def _():
            row_copy(-d).wait_recv()
            pl.when(gives)(lambda: relay(REACH + d).start())

    def await_past(d):
        pl.when(there(d))(lambda: relay(REACH + d).wait_recv())

    lane0 = lax.rem(lax.broadcasted_iota(jnp.int32, (width, 1), 0), cols)

    def shifted_sum(left, middle, right):
        left = jnp.where(lane0 == 0, 0.0, pltpu.roll(left, 1, 0))
        right = jnp.where(lane0 == cols - 1, 0.0, pltpu.roll(right, width - 1, 0))
        return left + middle + right

    def activate(slot):
        o = (side, 0, -side)[slot]
        if slot == 1:
            activate_row(slot, o)
        else:
            pl.when(there(o))(lambda: activate_row(slot, o))

    def activate_row(slot, o):
        at = 1 + o
        hidden = shifted_sum(acc[0, at], acc[1, at], acc[2, at]).astype(BF16).astype(F32)
        values = normed_silu(hidden, gain2).astype(BF16)
        if slot == 1:
            pk_second[...] = two_rows(peak_of(values.astype(F32)))
        second[slot, :, 0:C] = values

    def gift_copy():
        return pltpu.make_async_remote_copy(
            src_ref=gift_out, dst_ref=gift, send_sem=s_send, recv_sem=s_recv,
            device_id={"tm": t + 1}, device_id_type=MESH,
        )

    loads[2].wait()
    gain2 = g2[...].astype(F32).reshape(1, C)

    def second_conv(past_frames):
        rows = [second[slot] for slot in range(3)]
        both = jnp.concatenate(rows, axis=1)
        one = jnp.concatenate([row[cols:] if past_frames else row[0:cols] for row in rows], axis=1)

        def taps_at(i, k):
            return jnp.concatenate([w2[(i * 3 + 1 + o) * 3 + k] for o in (side, 0, -side)], axis=0)

        sums = []
        for k in range(3):
            main = dot(both, taps_at(0 if past_frames else 2, k))
            extra = dot(one, taps_at(1, k))
            if past_frames:
                sums.append(jnp.concatenate([main[0:cols] + extra, main[cols:]], axis=0))
            else:
                sums.append(jnp.concatenate([main[0:cols], main[cols:] + extra], axis=0))
        if past_frames:
            gift_out[...] = shifted_sum(*sums).astype(BF16)
        else:
            mix[...] = shifted_sum(*sums)

    def meet():
        for i in range(1, len(stages)):
            hear(i - 1)
            tell(i)

    last_core = t == T - 1
    alone = 2 * r >= R
    alone_rows = R - (R + 1) // 2
    sources = R + alone_rows * (T - 1)
    slot = jnp.where(last_core, r, R + (r - (R - alone_rows)) * (T - 1) + t)

    def peak_copy(peer):
        return pltpu.make_async_remote_copy(
            src_ref=pk_send, dst_ref=pk_recv.at[slot], send_sem=pk_ssem, recv_sem=pk_rsem,
            device_id={"rows": peer // T, "tm": lax.rem(peer, T)}, device_id_type=MESH,
        )

    def send_peaks():
        def step(i, carry):
            p = jnp.where(2 * r >= R, i, n - 2 - i)
            peak_copy(jnp.where(p >= me, p + 1, p)).start()
            return carry

        lax.fori_loop(0, n - 1, step, 0, unroll=n <= 16)

    def pass_peaks():
        return pltpu.make_async_remote_copy(
            src_ref=pk_send, dst_ref=pk_past, send_sem=pk_ssem, recv_sem=pp_rsem,
            device_id={"tm": t + 1}, device_id_type=MESH,
        )

    def peaks_of(count):
        return pltpu.make_async_remote_copy(
            src_ref=pk_recv.at[pl.ds(0, count)], dst_ref=pk_recv.at[pl.ds(0, count)],
            send_sem=pk_ssem, recv_sem=pk_rsem,
            device_id={"rows": r, "tm": lax.rem(t + 1, T)}, device_id_type=MESH,
        )

    shares = jnp.logical_or(last_core, alone)

    def heard():
        if stages:
            hear(len(stages) - 1)

    def beside(source, s, past_frames):
        pl.when(there(s))(lambda: contribute_side(source, s, past_frames))

    @pl.when(jnp.logical_not(takes))
    def _():
        await_row(-2)
        meet()
        await_row(side)
        await_row(2)
        beside(rows_in, side, False)
        await_row(-side)
        activate(0)
        beside(rows_in, -side, False)
        activate(1)
        activate(2)
        loads[4].wait()

        @pl.when(gives)
        def _():
            second_conv(True)
            gift_copy().start()

        second_conv(False)

    @pl.when(takes)
    def _():
        relay(REACH).wait_recv()
        contribute(hist, True)
        meet()
        await_row(-2)
        await_row(side)
        await_row(2)
        beside(rows_in, side, False)
        await_row(-side)
        beside(rows_in, -side, False)
        loads[4].wait()
        heard()
        await_past(-2)
        await_past(side)
        await_past(2)
        beside(hist, side, True)
        activate(0)
        await_past(-side)
        beside(hist, -side, True)
        activate(1)
        activate(2)
        second_conv(False)
        gift_copy().wait_recv()

    block = lat[...].astype(F32).reshape(width, C) + mix[...] + gift[...].astype(F32)
    block = block.astype(BF16)
    wide_block = block.astype(F32)
    merged[1] = packed(wide_block, cols)
    peaks = jnp.concatenate([pk_first[...], pk_second[...], two_rows(peak_of(wide_block))], axis=0)
    def edge_copy(d):
        slot = 1 - d
        return pltpu.make_async_remote_copy(
            src_ref=merged.at[1], dst_ref=merged.at[slot], send_sem=x3_send,
            recv_sem=x3_recv.at[slot // 2], device_id={"rows": r + d}, device_id_type=MESH,
        )

    def send_edges():
        for d in (side, -side):
            pl.when(there(d))(lambda d=d: edge_copy(d).start())

    def with_past():
        @pl.when(jnp.logical_and(takes, jnp.logical_not(alone)))
        def _():
            pass_peaks().wait_recv()
            pk_send[...] = jnp.maximum(pk_send[...].astype(F32), pk_past[...].astype(F32)).astype(BF16)

    pk_send[...] = peaks.astype(BF16)
    pl.when(jnp.logical_not(takes))(heard)
    low = jnp.logical_and(2 * r < R, takes)

    @pl.when(low)
    def _():
        send_edges()

    with_past()

    @pl.when(shares)
    def _():
        pk_recv[slot] = pk_send[...]
        send_peaks()

    @pl.when(jnp.logical_not(shares))
    def _():
        pass_peaks().start()

    @pl.when(jnp.logical_not(low))
    def _():
        send_edges()

    loads[5].wait()
    C2 = dec_ref.shape[2]
    own = dot_nt(up[...], block).reshape(3, 3, C2, width)
    base[0] = own[1] + own[2]
    base[1] = own[0] + own[1]
    lane = lax.rem(lax.broadcasted_iota(jnp.int32, (C2, width), 1), cols)

    def columns(sums):
        from_left = jnp.where(lane == 0, 0.0, pltpu.roll(sums[0], 1, 1))
        from_right = jnp.where(lane == cols - 1, 0.0, pltpu.roll(sums[2], width - 1, 1))
        even = from_left + sums[1] + sums[2]
        odd = sums[0] + sums[1] + from_right
        return jnp.concatenate([even, odd], axis=1).astype(BF16)

    def decode_row(half):
        f0, f1 = frames_of(merged.at[2 * half])
        rows = jnp.concatenate([f0, f1], axis=0)[:, 0:C]
        taps = up[half * 6 * C2 : (half * 6 + 3) * C2]
        sums = base[half] + dot_nt(taps, rows).reshape(3, C2, width)
        wide = dot(columns(sums), spread[...]).astype(BF16)
        for f in range(frames):
            dec_ref[f, half] = wide[:, f * 2 * cols : (f + 1) * 2 * cols]

    for d in (-1, 1):
        pl.when(there(d))(lambda d=d: edge_copy(-d).wait_recv())
        decode_row((1 + d) // 2)

    pl.when(shares)(lambda: peaks_of(sources - 1).wait_recv())
    pl.when(jnp.logical_not(shares))(lambda: peaks_of(sources).wait_recv())

    def take_peak(i, best):
        return jnp.maximum(best, pk_recv[i].astype(F32))

    best = lax.fori_loop(1, sources, take_peak, pk_recv[0].astype(F32), unroll=n <= 16)
    for i in range(3):
        peaks_ref[i : i + 1, 0:LANES] = best[2 * i : 2 * i + 1, :]
        peaks_ref[i : i + 1, LANES:C] = best[2 * i + 1 : 2 * i + 2, 0 : C - LANES]

    def sent(ref, sem, count, most):
        for c in range(1, most + 1):
            pl.when(count == c)(
                lambda c=c: pltpu.make_async_remote_copy(
                    src_ref=ref.at[pl.ds(0, c)], dst_ref=ref.at[pl.ds(0, c)], send_sem=sem, recv_sem=sem,
                    device_id={"rows": r, "tm": lax.rem(t + 1, T)}, device_id_type=MESH,
                ).wait_send()
            )

    sent(rows_in, x1_send, rows_near - 1, 2 * REACH)
    sent(merged, x3_send, jnp.minimum(r, 1) + jnp.minimum(R - 1 - r, 1), 2)

    @pl.when(gives)
    def _():
        sent(rows_in, rl_send, rows_near, 2 * REACH + 1)
        gift_copy().wait_send()

    pl.when(shares)(lambda: peaks_of(n - 1).wait_send())
    pl.when(jnp.logical_not(shares))(lambda: pass_peaks().wait_send())


def per_device(latent, gain_first, conv_first, gain_second, conv_second, conv_up):
    frames, rows, cols, C = latent.shape
    R, T = lax.axis_size("rows"), lax.axis_size("tm")
    C2 = conv_up.shape[2]
    n = R * T
    if rows != 1 or frames != 2 or 2 * C != 3 * LANES:
        raise ValueError("unsupported block")
    depth = 2 * LANES
    taps = conv_first.shape[0] * conv_first.shape[1] * conv_first.shape[2]
    vmem = pl.BlockSpec(memory_space=pltpu.VMEM)
    hbm = pl.BlockSpec(memory_space=pltpu.HBM)
    dma = pltpu.SemaphoreType.DMA
    span = 2 * REACH + 1
    width = frames * cols
    decoded, peaks = pl.pallas_call(
        functools.partial(kernel, R, T),
        out_shape=(
            pltpu.VMEM((frames, 2 * rows, C2, 2 * cols), BF16),
            pltpu.VMEM((3, C), F32),
        ),
        in_specs=[hbm] * 6,
        out_specs=(vmem, vmem),
        scratch_shapes=[
            pltpu.VMEM((frames, cols, C), BF16),
            pltpu.VMEM((C,), BF16),
            pltpu.VMEM((C,), BF16),
            pltpu.VMEM((span, 3, cols, LANES), BF16),
            pltpu.VMEM((span, 3, cols, LANES), BF16),
            pltpu.VMEM((3, 3, width, C), F32),
            pltpu.VMEM((width, C), F32),
            pltpu.VMEM((width, C), BF16),
            pltpu.VMEM((width, C), BF16),
            pltpu.VMEM((2, 3, C2, width), F32),
            pltpu.VMEM((3, width, depth), BF16),
            pltpu.VMEM((taps, depth, C), BF16),
            pltpu.VMEM((taps, depth, C), BF16),
            pltpu.VMEM((9 * C2, C), BF16),
            pltpu.VMEM((3, 3, cols, LANES), BF16),
            pltpu.VMEM((6, LANES), BF16),
            pltpu.VMEM((n + R, 6, LANES), BF16),
            pltpu.VMEM((6, LANES), BF16),
            pltpu.VMEM((2, LANES), F32),
            pltpu.VMEM((2, LANES), F32),
            dma((6,)),
            dma,
            dma((span - 1,)),
            dma,
            dma((span,)),
            dma,
            dma,
            dma,
            dma((2,)),
            dma,
            dma,
            dma,
            pltpu.SemaphoreType.REGULAR((max(1, len(stages_of(R))), 2)),
            pltpu.VMEM((2 * width, 2 * width), BF16),
        ],
        compiler_params=pltpu.CompilerParams(collective_id=0, has_side_effects=True, vmem_limit_bytes=54 * 2**20),
    )(
        latent.reshape(frames, cols, C),
        gain_first,
        conv_first.reshape(taps, C, C),
        gain_second,
        conv_second.reshape(taps, C, C),
        conv_up.reshape(9 * C2, C),
    )
    return pl.pallas_call(
        finish,
        out_shape=(
            jax.ShapeDtypeStruct(decoded.shape, BF16),
            jax.ShapeDtypeStruct(peaks.shape, F32),
        ),
        in_specs=[vmem, vmem],
        out_specs=(hbm, hbm),
        scratch_shapes=[dma((2,))],
        compiler_params=pltpu.CompilerParams(vmem_limit_bytes=2**20),
    )(decoded, peaks)


def solution(mesh):
    return jax.shard_map(
        per_device,
        mesh=mesh,
        in_specs=(P(("clip", "tm"), "rows", None, None), P(), P(), P(), P(), P()),
        out_specs=(P(("clip", "tm"), "rows", None, None), P("clip", None)),
        check_vma=False,
    )
```

```python
import functools

import jax
import jax.numpy as jnp
from jax import lax
from jax.experimental import pallas as pl
from jax.experimental.pallas import tpu as pltpu
from jax.sharding import PartitionSpec as P

MESH = pl.DeviceIdType.MESH
BF16 = jnp.bfloat16
F32 = jnp.float32
REACH = 2
LANES = 128


def stages_of(R):
    return [REACH << i for i in range(R.bit_length()) if (REACH << i) < R - 1]


def normed_silu(values, gain):
    scale = lax.rsqrt(jnp.mean(values * values, axis=-1, keepdims=True) + 1e-06)
    u = values * scale * gain
    return u / (1.0 + jnp.exp(-u))


def peak_of(values):
    return jnp.max(jnp.abs(values), axis=0, keepdims=True)


def dot(a, b):
    return jnp.dot(a, b, preferred_element_type=F32)


def dot_nt(a, b):
    return lax.dot_general(a, b, (((1,), (1,)), ((), ())), preferred_element_type=F32)


def packed(values, cols):
    low = values[:, 0:LANES].reshape(2, cols, LANES)
    high = jnp.concatenate([values[0:cols, LANES:], values[cols:, LANES:]], axis=1)
    return jnp.concatenate([low, high[None]], axis=0).astype(BF16)


def frames_of(buf):
    high = buf[2]
    turned = pltpu.roll(high.astype(F32), LANES // 2, 1).astype(BF16)
    return jnp.concatenate([buf[0], high], axis=1), jnp.concatenate([buf[1], turned], axis=1)


def finish(dec_in, peaks_in, dec_out, peaks_out, sem):
    copies = [
        pltpu.make_async_copy(dec_in, dec_out, sem.at[0]),
        pltpu.make_async_copy(peaks_in, peaks_out, sem.at[1]),
    ]
    for copy in copies:
        copy.start()
    for copy in copies:
        copy.wait()


def kernel(
    R, T, lat_hbm, g1_hbm, w1_hbm, g2_hbm, w2_hbm, up_hbm, dec_ref, peaks_ref,
    lat, g1, g2, rows_in, hist, acc, mix, gift, gift_out, base, second, w1, w2, up, merged,
    pk_send, pk_recv, pk_past, pk_first, pk_second,
    load_sem, x1_send, x1_recv, rl_send, rl_recv, s_send, s_recv, x3_send, x3_recv,
    pk_ssem, pk_rsem, pp_rsem, known, spread,
):
    r = lax.axis_index("rows")
    t = lax.axis_index("tm")
    n = R * T
    me = r * T + t
    frames, cols, C = lat.shape
    width = frames * cols

    def there(d):
        return jnp.logical_and(r + d >= 0, r + d < R)

    barrier = pltpu.get_barrier_semaphore()
    near = [(d, e) for d in range(-REACH, REACH + 1) for e in range(T) if (d, e) != (0, 0)]

    def greet(d, e):
        pl.semaphore_signal(
            barrier, inc=1, device_id={"rows": r + d, "tm": lax.rem(t + e, T)}, device_id_type=MESH
        )

    loads = [
        pltpu.make_async_copy(lat_hbm, lat, load_sem.at[0]),
        pltpu.make_async_copy(g1_hbm, g1, load_sem.at[1]),
        pltpu.make_async_copy(g2_hbm, g2, load_sem.at[2]),
        pltpu.make_async_copy(w1_hbm, w1.at[:, 0:C, :], load_sem.at[3]),
        pltpu.make_async_copy(w2_hbm, w2.at[:, 0:C, :], load_sem.at[4]),
        pltpu.make_async_copy(up_hbm, up, load_sem.at[5]),
    ]
    loads[0].start()
    loads[1].start()
    for d, e in near:
        pl.when(there(d))(functools.partial(greet, d, e))
    loads[3].start()
    loads[2].start()

    @pl.when(r == 0)
    def _():
        merged[0] = jnp.zeros_like(merged[0])

    @pl.when(r == R - 1)
    def _():
        merged[2] = jnp.zeros_like(merged[2])

    for d in (-2, -1, 1, 2):

        @pl.when(jnp.logical_not(there(d)))
        def _(d=d):
            rows_in[REACH + d] = jnp.zeros_like(rows_in[REACH + d])
            hist[REACH + d] = jnp.zeros_like(hist[REACH + d])

    second[...] = jnp.zeros_like(second)

    @pl.when(t == 0)
    def _():
        gift[...] = jnp.zeros_like(gift)

    pad = w1.shape[1] - C
    w1[:, C:, :] = jnp.zeros((w1.shape[0], pad, C), BF16)
    w2[:, C:, :] = jnp.zeros((w2.shape[0], pad, C), BF16)

    q = lax.broadcasted_iota(jnp.int32, (2 * width, 2 * width), 0)
    o = lax.broadcasted_iota(jnp.int32, (2 * width, 2 * width), 1)
    frame = lax.rem(lax.div(q, cols), frames)
    target = frame * (2 * cols) + 2 * lax.rem(q, cols) + lax.div(q, width)
    spread[...] = jnp.where(o == target, 1.0, 0.0).astype(BF16)

    loads[0].wait()
    loads[1].wait()
    gain1 = g1[...].astype(F32).reshape(1, C)
    own_first = normed_silu(lat[...].astype(F32).reshape(width, C), gain1)
    rows_in[REACH] = packed(own_first, cols)

    rows_near = 1 + jnp.minimum(r, REACH) + jnp.minimum(R - 1 - r, REACH)
    pl.semaphore_wait(barrier, rows_near * T - 1)

    side = 1 - 2 * lax.rem(r, 2)

    def row_copy(d):
        slot = REACH - d
        return pltpu.make_async_remote_copy(
            src_ref=rows_in.at[REACH], dst_ref=rows_in.at[slot], send_sem=x1_send,
            recv_sem=x1_recv.at[slot - jnp.where(slot > REACH, 1, 0)],
            device_id={"rows": r + d}, device_id_type=MESH,
        )

    for d in (side, 2 * side, -2 * side, -side):
        pl.when(there(d))(lambda d=d: row_copy(d).start())

    def relay(slot):
        return pltpu.make_async_remote_copy(
            src_ref=rows_in.at[slot], dst_ref=hist.at[slot], send_sem=rl_send,
            recv_sem=rl_recv.at[slot], device_id={"tm": t + 1}, device_id_type=MESH,
        )

    gives = t < T - 1
    takes = t > 0
    pl.when(gives)(lambda: relay(REACH).start())

    stages = stages_of(R)

    def tell(i):
        for way, d in enumerate((stages[i], -stages[i])):
            pl.when(there(d))(
                lambda way=way, d=d: pl.semaphore_signal(
                    known.at[i, way], inc=1, device_id={"rows": r + d}, device_id_type=MESH
                )
            )

    def hear(i):
        for way, d in enumerate((stages[i], -stages[i])):
            pl.when(there(-d))(lambda way=way: pl.semaphore_wait(known.at[i, way], 1))

    if stages:
        tell(0)

    def two_rows(row):
        rest = jnp.concatenate([row[:, LANES:C], jnp.zeros((1, 2 * LANES - C), F32)], axis=1)
        return jnp.concatenate([row[:, 0:LANES], rest], axis=0)

    pk_first[...] = two_rows(peak_of(own_first.astype(BF16).astype(F32)))

    def contribute(source, past_frames):
        f0, f1 = frames_of(source.at[REACH])
        both = jnp.concatenate([f0, f1], axis=0)
        tap = 0 if past_frames else 2
        for at in range(3):
            j = 2 - at
            for k in range(3):
                main = dot(both, w1[(tap * 3 + j) * 3 + k])
                extra = dot(f1 if past_frames else f0, w1[(3 + j) * 3 + k])
                early, late = main[0:cols], main[cols:]
                if past_frames:
                    acc[k, at, 0:cols] += early + extra
                    acc[k, at, cols:] += late
                else:
                    acc[k, at, 0:cols] = early
                    acc[k, at, cols:] = late + extra

    def contribute_side(source, s, past_frames):
        n0, n1 = frames_of(source.at[REACH + s])
        f0, f1 = frames_of(source.at[REACH + 2 * s])
        near_rows = jnp.concatenate([n0, n1], axis=0)
        all_rows = jnp.concatenate([n0, n1, f0, f1], axis=0)
        near_one, far_one = (n1, f1) if past_frames else (n0, f0)
        ones = jnp.concatenate([near_one, far_one], axis=0)
        tap = 0 if past_frames else 2
        mixed = slice(0, cols) if past_frames else slice(cols, width)
        for k in range(3):
            main = dot(all_rows, w1[(tap * 3 + 1 + s) * 3 + k])
            extra = dot(ones, w1[(3 + 1 + s) * 3 + k])
            acc[k, 1] += main[0:width]
            acc[k, 1, mixed] += extra[0:cols]
            acc[k, 1 + s] += main[width:] + dot(near_rows, w1[(tap * 3 + 1) * 3 + k])
            acc[k, 1 + s, mixed] += extra[cols:] + dot(near_one, w1[(3 + 1) * 3 + k])

    loads[3].wait()
    loads[4].start()
    loads[5].start()
    contribute(rows_in, False)

    def await_row(d):
        @pl.when(there(d))
        def _():
            row_copy(-d).wait_recv()
            pl.when(gives)(lambda: relay(REACH + d).start())

    def await_past(d):
        pl.when(there(d))(lambda: relay(REACH + d).wait_recv())

    lane0 = lax.rem(lax.broadcasted_iota(jnp.int32, (width, 1), 0), cols)

    def shifted_sum(left, middle, right):
        left = jnp.where(lane0 == 0, 0.0, pltpu.roll(left, 1, 0))
        right = jnp.where(lane0 == cols - 1, 0.0, pltpu.roll(right, width - 1, 0))
        return left + middle + right

    def activate(slot):
        o = (side, 0, -side)[slot]
        if slot == 1:
            activate_row(slot, o)
        else:
            pl.when(there(o))(lambda: activate_row(slot, o))

    def activate_row(slot, o):
        at = 1 + o
        hidden = shifted_sum(acc[0, at], acc[1, at], acc[2, at]).astype(BF16).astype(F32)
        values = normed_silu(hidden, gain2).astype(BF16)
        if slot == 1:
            pk_second[...] = two_rows(peak_of(values.astype(F32)))
        second[slot, :, 0:C] = values

    def gift_copy():
        return pltpu.make_async_remote_copy(
            src_ref=gift_out, dst_ref=gift, send_sem=s_send, recv_sem=s_recv,
            device_id={"tm": t + 1}, device_id_type=MESH,
        )

    loads[2].wait()
    gain2 = g2[...].astype(F32).reshape(1, C)

    def second_conv(past_frames):
        rows = [second[slot] for slot in range(3)]
        both = jnp.concatenate(rows, axis=1)
        one = jnp.concatenate([row[cols:] if past_frames else row[0:cols] for row in rows], axis=1)

        def taps_at(i, k):
            return jnp.concatenate([w2[(i * 3 + 1 + o) * 3 + k] for o in (side, 0, -side)], axis=0)

        sums = []
        for k in range(3):
            main = dot(both, taps_at(0 if past_frames else 2, k))
            extra = dot(one, taps_at(1, k))
            if past_frames:
                sums.append(jnp.concatenate([main[0:cols] + extra, main[cols:]], axis=0))
            else:
                sums.append(jnp.concatenate([main[0:cols], main[cols:] + extra], axis=0))
        if past_frames:
            gift_out[...] = shifted_sum(*sums).astype(BF16)
        else:
            mix[...] = shifted_sum(*sums)

    def meet():
        for i in range(1, len(stages)):
            hear(i - 1)
            tell(i)

    last_core = t == T - 1
    alone = 2 * r >= R
    alone_rows = R - (R + 1) // 2
    sources = R + alone_rows * (T - 1)
    slot = jnp.where(last_core, r, R + (r - (R - alone_rows)) * (T - 1) + t)

    def peak_copy(peer):
        return pltpu.make_async_remote_copy(
            src_ref=pk_send, dst_ref=pk_recv.at[slot], send_sem=pk_ssem, recv_sem=pk_rsem,
            device_id={"rows": peer // T, "tm": lax.rem(peer, T)}, device_id_type=MESH,
        )

    def send_peaks():
        def step(i, carry):
            p = jnp.where(2 * r >= R, i, n - 2 - i)
            peak_copy(jnp.where(p >= me, p + 1, p)).start()
            return carry

        lax.fori_loop(0, n - 1, step, 0, unroll=n <= 16)

    def pass_peaks():
        return pltpu.make_async_remote_copy(
            src_ref=pk_send, dst_ref=pk_past, send_sem=pk_ssem, recv_sem=pp_rsem,
            device_id={"tm": t + 1}, device_id_type=MESH,
        )

    def peaks_of(count):
        return pltpu.make_async_remote_copy(
            src_ref=pk_recv.at[pl.ds(0, count)], dst_ref=pk_recv.at[pl.ds(0, count)],
            send_sem=pk_ssem, recv_sem=pk_rsem,
            device_id={"rows": r, "tm": lax.rem(t + 1, T)}, device_id_type=MESH,
        )

    shares = jnp.logical_or(last_core, alone)

    def heard():
        if stages:
            hear(len(stages) - 1)

    def beside(source, s, past_frames):
        pl.when(there(s))(lambda: contribute_side(source, s, past_frames))

    @pl.when(jnp.logical_not(takes))
    def _():
        await_row(-2)
        meet()
        await_row(side)
        await_row(2)
        beside(rows_in, side, False)
        activate(0)
        await_row(-side)
        beside(rows_in, -side, False)
        activate(1)
        activate(2)
        loads[4].wait()

        @pl.when(gives)
        def _():
            second_conv(True)
            gift_copy().start()

        second_conv(False)

    @pl.when(takes)
    def _():
        relay(REACH).wait_recv()
        contribute(hist, True)
        meet()
        await_row(-2)
        await_row(side)
        await_row(2)
        beside(rows_in, side, False)
        await_row(-side)
        beside(rows_in, -side, False)
        loads[4].wait()
        heard()
        await_past(-2)
        await_past(side)
        await_past(2)
        beside(hist, side, True)
        activate(0)
        await_past(-side)
        beside(hist, -side, True)
        activate(1)
        activate(2)
        second_conv(False)
        gift_copy().wait_recv()

    block = lat[...].astype(F32).reshape(width, C) + mix[...] + gift[...].astype(F32)
    block = block.astype(BF16)
    wide_block = block.astype(F32)
    merged[1] = packed(wide_block, cols)
    peaks = jnp.concatenate([pk_first[...], pk_second[...], two_rows(peak_of(wide_block))], axis=0)
    def edge_copy(d):
        slot = 1 - d
        return pltpu.make_async_remote_copy(
            src_ref=merged.at[1], dst_ref=merged.at[slot], send_sem=x3_send,
            recv_sem=x3_recv.at[slot // 2], device_id={"rows": r + d}, device_id_type=MESH,
        )

    def send_edges():
        for d in (side, -side):
            pl.when(there(d))(lambda d=d: edge_copy(d).start())

    def with_past():
        @pl.when(jnp.logical_and(takes, jnp.logical_not(alone)))
        def _():
            pass_peaks().wait_recv()
            pk_send[...] = jnp.maximum(pk_send[...].astype(F32), pk_past[...].astype(F32)).astype(BF16)

    pk_send[...] = peaks.astype(BF16)
    pl.when(jnp.logical_not(takes))(heard)
    low = jnp.logical_and(2 * r < R, takes)

    @pl.when(low)
    def _():
        send_edges()

    with_past()

    @pl.when(shares)
    def _():
        pk_recv[slot] = pk_send[...]
        send_peaks()

    @pl.when(jnp.logical_not(shares))
    def _():
        pass_peaks().start()

    @pl.when(jnp.logical_not(low))
    def _():
        send_edges()

    loads[5].wait()
    C2 = dec_ref.shape[2]
    own = dot_nt(up[...], block).reshape(3, 3, C2, width)
    base[0] = own[1] + own[2]
    base[1] = own[0] + own[1]
    lane = lax.rem(lax.broadcasted_iota(jnp.int32, (C2, width), 1), cols)

    def columns(sums):
        from_left = jnp.where(lane == 0, 0.0, pltpu.roll(sums[0], 1, 1))
        from_right = jnp.where(lane == cols - 1, 0.0, pltpu.roll(sums[2], width - 1, 1))
        even = from_left + sums[1] + sums[2]
        odd = sums[0] + sums[1] + from_right
        return jnp.concatenate([even, odd], axis=1).astype(BF16)

    def decode_row(half):
        f0, f1 = frames_of(merged.at[2 * half])
        rows = jnp.concatenate([f0, f1], axis=0)[:, 0:C]
        taps = up[half * 6 * C2 : (half * 6 + 3) * C2]
        sums = base[half] + dot_nt(taps, rows).reshape(3, C2, width)
        wide = dot(columns(sums), spread[...]).astype(BF16)
        for f in range(frames):
            dec_ref[f, half] = wide[:, f * 2 * cols : (f + 1) * 2 * cols]

    for d in (-1, 1):
        pl.when(there(d))(lambda d=d: edge_copy(-d).wait_recv())
        decode_row((1 + d) // 2)

    pl.when(shares)(lambda: peaks_of(sources - 1).wait_recv())
    pl.when(jnp.logical_not(shares))(lambda: peaks_of(sources).wait_recv())

    def take_peak(i, best):
        return jnp.maximum(best, pk_recv[i].astype(F32))

    best = lax.fori_loop(1, sources, take_peak, pk_recv[0].astype(F32), unroll=n <= 16)
    for i in range(3):
        peaks_ref[i : i + 1, 0:LANES] = best[2 * i : 2 * i + 1, :]
        peaks_ref[i : i + 1, LANES:C] = best[2 * i + 1 : 2 * i + 2, 0 : C - LANES]

    def sent(ref, sem, count, most):
        for c in range(1, most + 1):
            pl.when(count == c)(
                lambda c=c: pltpu.make_async_remote_copy(
                    src_ref=ref.at[pl.ds(0, c)], dst_ref=ref.at[pl.ds(0, c)], send_sem=sem, recv_sem=sem,
                    device_id={"rows": r, "tm": lax.rem(t + 1, T)}, device_id_type=MESH,
                ).wait_send()
            )

    sent(rows_in, x1_send, rows_near - 1, 2 * REACH)
    sent(merged, x3_send, jnp.minimum(r, 1) + jnp.minimum(R - 1 - r, 1), 2)

    @pl.when(gives)
    def _():
        sent(rows_in, rl_send, rows_near, 2 * REACH + 1)
        gift_copy().wait_send()

    pl.when(shares)(lambda: peaks_of(n - 1).wait_send())
    pl.when(jnp.logical_not(shares))(lambda: pass_peaks().wait_send())


def per_device(latent, gain_first, conv_first, gain_second, conv_second, conv_up):
    frames, rows, cols, C = latent.shape
    R, T = lax.axis_size("rows"), lax.axis_size("tm")
    C2 = conv_up.shape[2]
    n = R * T
    if rows != 1 or frames != 2 or 2 * C != 3 * LANES:
        raise ValueError("unsupported block")
    depth = 2 * LANES
    taps = conv_first.shape[0] * conv_first.shape[1] * conv_first.shape[2]
    vmem = pl.BlockSpec(memory_space=pltpu.VMEM)
    hbm = pl.BlockSpec(memory_space=pltpu.HBM)
    dma = pltpu.SemaphoreType.DMA
    span = 2 * REACH + 1
    width = frames * cols
    decoded, peaks = pl.pallas_call(
        functools.partial(kernel, R, T),
        out_shape=(
            pltpu.VMEM((frames, 2 * rows, C2, 2 * cols), BF16),
            pltpu.VMEM((3, C), F32),
        ),
        in_specs=[hbm] * 6,
        out_specs=(vmem, vmem),
        scratch_shapes=[
            pltpu.VMEM((frames, cols, C), BF16),
            pltpu.VMEM((C,), BF16),
            pltpu.VMEM((C,), BF16),
            pltpu.VMEM((span, 3, cols, LANES), BF16),
            pltpu.VMEM((span, 3, cols, LANES), BF16),
            pltpu.VMEM((3, 3, width, C), F32),
            pltpu.VMEM((width, C), F32),
            pltpu.VMEM((width, C), BF16),
            pltpu.VMEM((width, C), BF16),
            pltpu.VMEM((2, 3, C2, width), F32),
            pltpu.VMEM((3, width, depth), BF16),
            pltpu.VMEM((taps, depth, C), BF16),
            pltpu.VMEM((taps, depth, C), BF16),
            pltpu.VMEM((9 * C2, C), BF16),
            pltpu.VMEM((3, 3, cols, LANES), BF16),
            pltpu.VMEM((6, LANES), BF16),
            pltpu.VMEM((n + R, 6, LANES), BF16),
            pltpu.VMEM((6, LANES), BF16),
            pltpu.VMEM((2, LANES), F32),
            pltpu.VMEM((2, LANES), F32),
            dma((6,)),
            dma,
            dma((span - 1,)),
            dma,
            dma((span,)),
            dma,
            dma,
            dma,
            dma((2,)),
            dma,
            dma,
            dma,
            pltpu.SemaphoreType.REGULAR((max(1, len(stages_of(R))), 2)),
            pltpu.VMEM((2 * width, 2 * width), BF16),
        ],
        compiler_params=pltpu.CompilerParams(collective_id=0, has_side_effects=True, vmem_limit_bytes=54 * 2**20),
    )(
        latent.reshape(frames, cols, C),
        gain_first,
        conv_first.reshape(taps, C, C),
        gain_second,
        conv_second.reshape(taps, C, C),
        conv_up.reshape(9 * C2, C),
    )
    return pl.pallas_call(
        finish,
        out_shape=(
            jax.ShapeDtypeStruct(decoded.shape, BF16),
            jax.ShapeDtypeStruct(peaks.shape, F32),
        ),
        in_specs=[vmem, vmem],
        out_specs=(hbm, hbm),
        scratch_shapes=[dma((2,))],
        compiler_params=pltpu.CompilerParams(vmem_limit_bytes=2**20),
    )(decoded, peaks)


def solution(mesh):
    return jax.shard_map(
        per_device,
        mesh=mesh,
        in_specs=(P(("clip", "tm"), "rows", None, None), P(), P(), P(), P(), P()),
        out_specs=(P(("clip", "tm"), "rows", None, None), P("clip", None)),
        check_vma=False,
    )
```

```python
import functools

import jax
import jax.numpy as jnp
from jax import lax
from jax.experimental import pallas as pl
from jax.experimental.pallas import tpu as pltpu
from jax.sharding import PartitionSpec as P

MESH = pl.DeviceIdType.MESH
BF16 = jnp.bfloat16
F32 = jnp.float32
REACH = 2
LANES = 128


def stages_of(R):
    return [REACH << i for i in range(R.bit_length()) if (REACH << i) < R - 1]


def normed_silu(values, gain):
    scale = lax.rsqrt(jnp.mean(values * values, axis=-1, keepdims=True) + 1e-06)
    u = values * scale * gain
    return u / (1.0 + jnp.exp(-u))


def peak_of(values):
    return jnp.max(jnp.abs(values), axis=0, keepdims=True)


def dot(a, b):
    return jnp.dot(a, b, preferred_element_type=F32)


def dot_nt(a, b):
    return lax.dot_general(a, b, (((1,), (1,)), ((), ())), preferred_element_type=F32)


def packed(values, cols):
    low = values[:, 0:LANES].reshape(2, cols, LANES)
    high = jnp.concatenate([values[0:cols, LANES:], values[cols:, LANES:]], axis=1)
    return jnp.concatenate([low, high[None]], axis=0).astype(BF16)


def frames_of(buf):
    high = buf[2]
    turned = pltpu.roll(high.astype(F32), LANES // 2, 1).astype(BF16)
    return jnp.concatenate([buf[0], high], axis=1), jnp.concatenate([buf[1], turned], axis=1)


def finish(dec_in, peaks_in, dec_out, peaks_out, sem):
    copies = [
        pltpu.make_async_copy(dec_in, dec_out, sem.at[0]),
        pltpu.make_async_copy(peaks_in, peaks_out, sem.at[1]),
    ]
    for copy in copies:
        copy.start()
    for copy in copies:
        copy.wait()


def kernel(
    R, T, lat_hbm, g1_hbm, w1_hbm, g2_hbm, w2_hbm, up_hbm, dec_ref, peaks_ref,
    lat, g1, g2, rows_in, hist, acc, mix, gift, gift_out, base, second, w1, w2, up, merged,
    pk_send, pk_recv, pk_first, pk_second,
    load_sem, x1_send, x1_recv, rl_send, rl_recv, s_send, s_recv, x3_send, x3_recv,
    pk_ssem, pk_rsem, known, spread,
):
    r = lax.axis_index("rows")
    t = lax.axis_index("tm")
    n = R * T
    me = r * T + t
    frames, cols, C = lat.shape
    width = frames * cols

    def there(d):
        return jnp.logical_and(r + d >= 0, r + d < R)

    barrier = pltpu.get_barrier_semaphore()
    near = [(d, e) for d in range(-REACH, REACH + 1) for e in range(T) if (d, e) != (0, 0)]

    def greet(d, e):
        pl.semaphore_signal(
            barrier, inc=1, device_id={"rows": r + d, "tm": lax.rem(t + e, T)}, device_id_type=MESH
        )

    loads = [
        pltpu.make_async_copy(lat_hbm, lat, load_sem.at[0]),
        pltpu.make_async_copy(g1_hbm, g1, load_sem.at[1]),
        pltpu.make_async_copy(g2_hbm, g2, load_sem.at[2]),
        pltpu.make_async_copy(w1_hbm, w1.at[:, 0:C, :], load_sem.at[3]),
        pltpu.make_async_copy(w2_hbm, w2.at[:, 0:C, :], load_sem.at[4]),
        pltpu.make_async_copy(up_hbm, up, load_sem.at[5]),
    ]
    loads[0].start()
    loads[1].start()
    for d, e in near:
        pl.when(there(d))(functools.partial(greet, d, e))
    loads[3].start()
    loads[2].start()

    @pl.when(r == 0)
    def _():
        merged[0] = jnp.zeros_like(merged[0])

    @pl.when(r == R - 1)
    def _():
        merged[2] = jnp.zeros_like(merged[2])

    for d in (-2, -1, 1, 2):

        @pl.when(jnp.logical_not(there(d)))
        def _(d=d):
            rows_in[REACH + d] = jnp.zeros_like(rows_in[REACH + d])
            hist[REACH + d] = jnp.zeros_like(hist[REACH + d])

    second[...] = jnp.zeros_like(second)

    @pl.when(t == 0)
    def _():
        gift[...] = jnp.zeros_like(gift)

    pad = w1.shape[1] - C
    w1[:, C:, :] = jnp.zeros((w1.shape[0], pad, C), BF16)
    w2[:, C:, :] = jnp.zeros((w2.shape[0], pad, C), BF16)

    q = lax.broadcasted_iota(jnp.int32, (2 * width, 2 * width), 0)
    o = lax.broadcasted_iota(jnp.int32, (2 * width, 2 * width), 1)
    frame = lax.rem(lax.div(q, cols), frames)
    target = frame * (2 * cols) + 2 * lax.rem(q, cols) + lax.div(q, width)
    spread[...] = jnp.where(o == target, 1.0, 0.0).astype(BF16)

    loads[0].wait()
    loads[1].wait()
    gain1 = g1[...].astype(F32).reshape(1, C)
    own_first = normed_silu(lat[...].astype(F32).reshape(width, C), gain1)
    rows_in[REACH] = packed(own_first, cols)

    rows_near = 1 + jnp.minimum(r, REACH) + jnp.minimum(R - 1 - r, REACH)
    pl.semaphore_wait(barrier, rows_near * T - 1)

    side = 1 - 2 * lax.rem(r, 2)

    def row_copy(d):
        slot = REACH - d
        return pltpu.make_async_remote_copy(
            src_ref=rows_in.at[REACH], dst_ref=rows_in.at[slot], send_sem=x1_send,
            recv_sem=x1_recv.at[slot - jnp.where(slot > REACH, 1, 0)],
            device_id={"rows": r + d}, device_id_type=MESH,
        )

    for d in (side, 2 * side, -2 * side, -side):
        pl.when(there(d))(lambda d=d: row_copy(d).start())

    def relay(slot):
        return pltpu.make_async_remote_copy(
            src_ref=rows_in.at[slot], dst_ref=hist.at[slot], send_sem=rl_send,
            recv_sem=rl_recv.at[slot], device_id={"tm": t + 1}, device_id_type=MESH,
        )

    gives = t < T - 1
    takes = t > 0
    pl.when(gives)(lambda: relay(REACH).start())

    stages = stages_of(R)

    def tell(i):
        for way, d in enumerate((stages[i], -stages[i])):
            pl.when(there(d))(
                lambda way=way, d=d: pl.semaphore_signal(
                    known.at[i, way], inc=1, device_id={"rows": r + d}, device_id_type=MESH
                )
            )

    def hear(i):
        for way, d in enumerate((stages[i], -stages[i])):
            pl.when(there(-d))(lambda way=way: pl.semaphore_wait(known.at[i, way], 1))

    if stages:
        tell(0)

    def two_rows(row):
        rest = jnp.concatenate([row[:, LANES:C], jnp.zeros((1, 2 * LANES - C), F32)], axis=1)
        return jnp.concatenate([row[:, 0:LANES], rest], axis=0)

    pk_first[...] = two_rows(peak_of(own_first.astype(BF16).astype(F32)))

    def contribute(source, past_frames):
        f0, f1 = frames_of(source.at[REACH])
        both = jnp.concatenate([f0, f1], axis=0)
        tap = 0 if past_frames else 2
        for at in range(3):
            j = 2 - at
            for k in range(3):
                main = dot(both, w1[(tap * 3 + j) * 3 + k])
                extra = dot(f1 if past_frames else f0, w1[(3 + j) * 3 + k])
                early, late = main[0:cols], main[cols:]
                if past_frames:
                    acc[k, at, 0:cols] += early + extra
                    acc[k, at, cols:] += late
                else:
                    acc[k, at, 0:cols] = early
                    acc[k, at, cols:] = late + extra

    def contribute_side(source, s, past_frames):
        n0, n1 = frames_of(source.at[REACH + s])
        f0, f1 = frames_of(source.at[REACH + 2 * s])
        near_rows = jnp.concatenate([n0, n1], axis=0)
        all_rows = jnp.concatenate([n0, n1, f0, f1], axis=0)
        near_one, far_one = (n1, f1) if past_frames else (n0, f0)
        ones = jnp.concatenate([near_one, far_one], axis=0)
        tap = 0 if past_frames else 2
        mixed = slice(0, cols) if past_frames else slice(cols, width)
        for k in range(3):
            main = dot(all_rows, w1[(tap * 3 + 1 + s) * 3 + k])
            extra = dot(ones, w1[(3 + 1 + s) * 3 + k])
            acc[k, 1] += main[0:width]
            acc[k, 1, mixed] += extra[0:cols]
            acc[k, 1 + s] += main[width:] + dot(near_rows, w1[(tap * 3 + 1) * 3 + k])
            acc[k, 1 + s, mixed] += extra[cols:] + dot(near_one, w1[(3 + 1) * 3 + k])

    loads[3].wait()
    loads[4].start()
    loads[5].start()
    contribute(rows_in, False)

    def await_row(d):
        @pl.when(there(d))
        def _():
            row_copy(-d).wait_recv()
            pl.when(gives)(lambda: relay(REACH + d).start())

    def await_past(d):
        pl.when(there(d))(lambda: relay(REACH + d).wait_recv())

    lane0 = lax.rem(lax.broadcasted_iota(jnp.int32, (width, 1), 0), cols)

    def shifted_sum(left, middle, right):
        left = jnp.where(lane0 == 0, 0.0, pltpu.roll(left, 1, 0))
        right = jnp.where(lane0 == cols - 1, 0.0, pltpu.roll(right, width - 1, 0))
        return left + middle + right

    def activate(slot):
        o = (side, 0, -side)[slot]
        if slot == 1:
            activate_row(slot, o)
        else:
            pl.when(there(o))(lambda: activate_row(slot, o))

    def activate_row(slot, o):
        at = 1 + o
        hidden = shifted_sum(acc[0, at], acc[1, at], acc[2, at]).astype(BF16).astype(F32)
        values = normed_silu(hidden, gain2).astype(BF16)
        if slot == 1:
            pk_second[...] = two_rows(peak_of(values.astype(F32)))
        second[slot, :, 0:C] = values

    def gift_copy():
        return pltpu.make_async_remote_copy(
            src_ref=gift_out, dst_ref=gift, send_sem=s_send, recv_sem=s_recv,
            device_id={"tm": t + 1}, device_id_type=MESH,
        )

    loads[2].wait()
    gain2 = g2[...].astype(F32).reshape(1, C)

    def second_conv(past_frames):
        rows = [second[slot] for slot in range(3)]
        both = jnp.concatenate(rows, axis=1)
        one = jnp.concatenate([row[cols:] if past_frames else row[0:cols] for row in rows], axis=1)

        def taps_at(i, k):
            return jnp.concatenate([w2[(i * 3 + 1 + o) * 3 + k] for o in (side, 0, -side)], axis=0)

        sums = []
        for k in range(3):
            main = dot(both, taps_at(0 if past_frames else 2, k))
            extra = dot(one, taps_at(1, k))
            if past_frames:
                sums.append(jnp.concatenate([main[0:cols] + extra, main[cols:]], axis=0))
            else:
                sums.append(jnp.concatenate([main[0:cols], main[cols:] + extra], axis=0))
        if past_frames:
            gift_out[...] = shifted_sum(*sums).astype(BF16)
        else:
            mix[...] = shifted_sum(*sums)

    def meet():
        for i in range(1, len(stages)):
            hear(i - 1)
            tell(i)

    def peak_copy(peer):
        return pltpu.make_async_remote_copy(
            src_ref=pk_send, dst_ref=pk_recv.at[me - jnp.where(me > peer, 1, 0)],
            send_sem=pk_ssem, recv_sem=pk_rsem,
            device_id={"rows": peer // T, "tm": lax.rem(peer, T)}, device_id_type=MESH,
        )

    def send_peaks():
        def step(i, carry):
            p = jnp.where(2 * r >= R, i, n - 2 - i)
            peak_copy(jnp.where(p >= me, p + 1, p)).start()
            return carry

        lax.fori_loop(0, n - 1, step, 0, unroll=n <= 16)

    def all_peaks():
        return pltpu.make_async_remote_copy(
            src_ref=pk_recv, dst_ref=pk_recv, send_sem=pk_ssem, recv_sem=pk_rsem,
            device_id={"rows": r, "tm": lax.rem(t + 1, T)}, device_id_type=MESH,
        )

    def heard():
        if stages:
            hear(len(stages) - 1)

    def beside(source, s, past_frames):
        pl.when(there(s))(lambda: contribute_side(source, s, past_frames))

    @pl.when(jnp.logical_not(takes))
    def _():
        await_row(-2)
        meet()
        await_row(side)
        await_row(2)
        beside(rows_in, side, False)
        activate(0)
        await_row(-side)
        beside(rows_in, -side, False)
        activate(1)
        activate(2)
        loads[4].wait()

        @pl.when(gives)
        def _():
            second_conv(True)
            gift_copy().start()

        second_conv(False)

    @pl.when(takes)
    def _():
        relay(REACH).wait_recv()
        contribute(hist, True)
        meet()
        await_row(-2)
        await_row(side)
        await_row(2)
        beside(rows_in, side, False)
        await_row(-side)
        beside(rows_in, -side, False)
        loads[4].wait()
        heard()
        await_past(-2)
        await_past(side)
        await_past(2)
        beside(hist, side, True)
        activate(0)
        await_past(-side)
        beside(hist, -side, True)
        activate(1)
        activate(2)
        second_conv(False)
        gift_copy().wait_recv()

    block = lat[...].astype(F32).reshape(width, C) + mix[...] + gift[...].astype(F32)
    block = block.astype(BF16)
    wide_block = block.astype(F32)
    merged[1] = packed(wide_block, cols)
    peaks = jnp.concatenate([pk_first[...], pk_second[...], two_rows(peak_of(wide_block))], axis=0)
    pk_send[...] = peaks.astype(BF16)
    pl.when(jnp.logical_not(takes))(heard)
    send_peaks()

    def edge_copy(d):
        slot = 1 - d
        return pltpu.make_async_remote_copy(
            src_ref=merged.at[1], dst_ref=merged.at[slot], send_sem=x3_send,
            recv_sem=x3_recv.at[slot // 2], device_id={"rows": r + d}, device_id_type=MESH,
        )

    for d in (side, -side):
        pl.when(there(d))(lambda d=d: edge_copy(d).start())

    loads[5].wait()
    C2 = dec_ref.shape[2]
    own = dot_nt(up[...], block).reshape(3, 3, C2, width)
    base[0] = own[1] + own[2]
    base[1] = own[0] + own[1]
    lane = lax.rem(lax.broadcasted_iota(jnp.int32, (C2, width), 1), cols)

    def columns(sums):
        from_left = jnp.where(lane == 0, 0.0, pltpu.roll(sums[0], 1, 1))
        from_right = jnp.where(lane == cols - 1, 0.0, pltpu.roll(sums[2], width - 1, 1))
        even = from_left + sums[1] + sums[2]
        odd = sums[0] + sums[1] + from_right
        return jnp.concatenate([even, odd], axis=1).astype(BF16)

    def decode_row(half):
        f0, f1 = frames_of(merged.at[2 * half])
        rows = jnp.concatenate([f0, f1], axis=0)[:, 0:C]
        taps = up[half * 6 * C2 : (half * 6 + 3) * C2]
        sums = base[half] + dot_nt(taps, rows).reshape(3, C2, width)
        wide = dot(columns(sums), spread[...]).astype(BF16)
        for f in range(frames):
            dec_ref[f, half] = wide[:, f * 2 * cols : (f + 1) * 2 * cols]

    for d in (-1, 1):
        pl.when(there(d))(lambda d=d: edge_copy(-d).wait_recv())
        decode_row((1 + d) // 2)

    all_peaks().wait_recv()

    def take_peak(i, best):
        return jnp.maximum(best, pk_recv[i].astype(F32))

    best = lax.fori_loop(0, n - 1, take_peak, peaks, unroll=n <= 16)
    for i in range(3):
        peaks_ref[i : i + 1, 0:LANES] = best[2 * i : 2 * i + 1, :]
        peaks_ref[i : i + 1, LANES:C] = best[2 * i + 1 : 2 * i + 2, 0 : C - LANES]

    def sent(ref, sem, count, most):
        for c in range(1, most + 1):
            pl.when(count == c)(
                lambda c=c: pltpu.make_async_remote_copy(
                    src_ref=ref.at[pl.ds(0, c)], dst_ref=ref.at[pl.ds(0, c)], send_sem=sem, recv_sem=sem,
                    device_id={"rows": r, "tm": lax.rem(t + 1, T)}, device_id_type=MESH,
                ).wait_send()
            )

    sent(rows_in, x1_send, rows_near - 1, 2 * REACH)
    sent(merged, x3_send, jnp.minimum(r, 1) + jnp.minimum(R - 1 - r, 1), 2)

    @pl.when(gives)
    def _():
        sent(rows_in, rl_send, rows_near, 2 * REACH + 1)
        gift_copy().wait_send()

    all_peaks().wait_send()


def per_device(latent, gain_first, conv_first, gain_second, conv_second, conv_up):
    frames, rows, cols, C = latent.shape
    R, T = lax.axis_size("rows"), lax.axis_size("tm")
    C2 = conv_up.shape[2]
    n = R * T
    if rows != 1 or frames != 2 or 2 * C != 3 * LANES:
        raise ValueError("unsupported block")
    depth = 2 * LANES
    taps = conv_first.shape[0] * conv_first.shape[1] * conv_first.shape[2]
    vmem = pl.BlockSpec(memory_space=pltpu.VMEM)
    hbm = pl.BlockSpec(memory_space=pltpu.HBM)
    dma = pltpu.SemaphoreType.DMA
    span = 2 * REACH + 1
    width = frames * cols
    decoded, peaks = pl.pallas_call(
        functools.partial(kernel, R, T),
        out_shape=(
            pltpu.VMEM((frames, 2 * rows, C2, 2 * cols), BF16),
            pltpu.VMEM((3, C), F32),
        ),
        in_specs=[hbm] * 6,
        out_specs=(vmem, vmem),
        scratch_shapes=[
            pltpu.VMEM((frames, cols, C), BF16),
            pltpu.VMEM((C,), BF16),
            pltpu.VMEM((C,), BF16),
            pltpu.VMEM((span, 3, cols, LANES), BF16),
            pltpu.VMEM((span, 3, cols, LANES), BF16),
            pltpu.VMEM((3, 3, width, C), F32),
            pltpu.VMEM((width, C), F32),
            pltpu.VMEM((width, C), BF16),
            pltpu.VMEM((width, C), BF16),
            pltpu.VMEM((2, 3, C2, width), F32),
            pltpu.VMEM((3, width, depth), BF16),
            pltpu.VMEM((taps, depth, C), BF16),
            pltpu.VMEM((taps, depth, C), BF16),
            pltpu.VMEM((9 * C2, C), BF16),
            pltpu.VMEM((3, 3, cols, LANES), BF16),
            pltpu.VMEM((6, LANES), BF16),
            pltpu.VMEM((n - 1, 6, LANES), BF16),
            pltpu.VMEM((2, LANES), F32),
            pltpu.VMEM((2, LANES), F32),
            dma((6,)),
            dma,
            dma((span - 1,)),
            dma,
            dma((span,)),
            dma,
            dma,
            dma,
            dma((2,)),
            dma,
            dma,
            pltpu.SemaphoreType.REGULAR((max(1, len(stages_of(R))), 2)),
            pltpu.VMEM((2 * width, 2 * width), BF16),
        ],
        compiler_params=pltpu.CompilerParams(collective_id=0, has_side_effects=True, vmem_limit_bytes=54 * 2**20),
    )(
        latent.reshape(frames, cols, C),
        gain_first,
        conv_first.reshape(taps, C, C),
        gain_second,
        conv_second.reshape(taps, C, C),
        conv_up.reshape(9 * C2, C),
    )
    return pl.pallas_call(
        finish,
        out_shape=(
            jax.ShapeDtypeStruct(decoded.shape, BF16),
            jax.ShapeDtypeStruct(peaks.shape, F32),
        ),
        in_specs=[vmem, vmem],
        out_specs=(hbm, hbm),
        scratch_shapes=[dma((2,))],
        compiler_params=pltpu.CompilerParams(vmem_limit_bytes=2**20),
    )(decoded, peaks)


def solution(mesh):
    return jax.shard_map(
        per_device,
        mesh=mesh,
        in_specs=(P(("clip", "tm"), "rows", None, None), P(), P(), P(), P(), P()),
        out_specs=(P(("clip", "tm"), "rows", None, None), P("clip", None)),
        check_vma=False,
    )
```

```python
import functools

import jax
import jax.numpy as jnp
from jax import lax
from jax.experimental import pallas as pl
from jax.experimental.pallas import tpu as pltpu
from jax.sharding import PartitionSpec as P

MESH = pl.DeviceIdType.MESH
BF16 = jnp.bfloat16
F32 = jnp.float32
REACH = 2
LANES = 128


def stages_of(R):
    return [REACH << i for i in range(R.bit_length()) if (REACH << i) < R - 1]


def normed_silu(values, gain):
    scale = lax.rsqrt(jnp.mean(values * values, axis=-1, keepdims=True) + 1e-06)
    u = values * scale * gain
    return u / (1.0 + jnp.exp(-u))


def peak_of(values):
    return jnp.max(jnp.abs(values), axis=0, keepdims=True)


def dot(a, b):
    return jnp.dot(a, b, preferred_element_type=F32)


def dot_nt(a, b):
    return lax.dot_general(a, b, (((1,), (1,)), ((), ())), preferred_element_type=F32)


def packed(values, cols):
    low = values[:, 0:LANES].reshape(2, cols, LANES)
    high = jnp.concatenate([values[0:cols, LANES:], values[cols:, LANES:]], axis=1)
    return jnp.concatenate([low, high[None]], axis=0).astype(BF16)


def frames_of(buf):
    high = buf[2]
    turned = pltpu.roll(high.astype(F32), LANES // 2, 1).astype(BF16)
    return jnp.concatenate([buf[0], high], axis=1), jnp.concatenate([buf[1], turned], axis=1)


def finish(dec_in, peaks_in, dec_out, peaks_out, sem):
    copies = [
        pltpu.make_async_copy(dec_in, dec_out, sem.at[0]),
        pltpu.make_async_copy(peaks_in, peaks_out, sem.at[1]),
    ]
    for copy in copies:
        copy.start()
    for copy in copies:
        copy.wait()


def kernel(
    R, T, lat_hbm, g1_hbm, w1_hbm, g2_hbm, w2_hbm, up_hbm, dec_ref, peaks_ref,
    lat, g1, g2, rows_in, hist, acc, mix, gift, gift_out, base, second, w1, w2, up, merged,
    pk_send, pk_recv, pk_past, pk_first, pk_second,
    load_sem, x1_send, x1_recv, rl_send, rl_recv, s_send, s_recv, x3_send, x3_recv,
    pk_ssem, pk_rsem, pp_rsem, known, spread,
):
    r = lax.axis_index("rows")
    t = lax.axis_index("tm")
    n = R * T
    me = r * T + t
    frames, cols, C = lat.shape
    width = frames * cols

    def there(d):
        return jnp.logical_and(r + d >= 0, r + d < R)

    barrier = pltpu.get_barrier_semaphore()
    near = [(d, e) for d in range(-REACH, REACH + 1) for e in range(T) if (d, e) != (0, 0)]

    def greet(d, e):
        pl.semaphore_signal(
            barrier, inc=1, device_id={"rows": r + d, "tm": lax.rem(t + e, T)}, device_id_type=MESH
        )

    loads = [
        pltpu.make_async_copy(lat_hbm, lat, load_sem.at[0]),
        pltpu.make_async_copy(g1_hbm, g1, load_sem.at[1]),
        pltpu.make_async_copy(g2_hbm, g2, load_sem.at[2]),
        pltpu.make_async_copy(w1_hbm, w1.at[:, 0:C, :], load_sem.at[3]),
        pltpu.make_async_copy(w2_hbm, w2.at[:, 0:C, :], load_sem.at[4]),
        pltpu.make_async_copy(up_hbm, up, load_sem.at[5]),
    ]
    loads[0].start()
    loads[1].start()
    for d, e in near:
        pl.when(there(d))(functools.partial(greet, d, e))
    loads[3].start()
    loads[2].start()

    @pl.when(r == 0)
    def _():
        merged[0] = jnp.zeros_like(merged[0])

    @pl.when(r == R - 1)
    def _():
        merged[2] = jnp.zeros_like(merged[2])

    for d in (-2, -1, 1, 2):

        @pl.when(jnp.logical_not(there(d)))
        def _(d=d):
            rows_in[REACH + d] = jnp.zeros_like(rows_in[REACH + d])
            hist[REACH + d] = jnp.zeros_like(hist[REACH + d])

    second[...] = jnp.zeros_like(second)

    @pl.when(t == 0)
    def _():
        gift[...] = jnp.zeros_like(gift)

    pad = w1.shape[1] - C
    w1[:, C:, :] = jnp.zeros((w1.shape[0], pad, C), BF16)
    w2[:, C:, :] = jnp.zeros((w2.shape[0], pad, C), BF16)

    q = lax.broadcasted_iota(jnp.int32, (2 * width, 2 * width), 0)
    o = lax.broadcasted_iota(jnp.int32, (2 * width, 2 * width), 1)
    frame = lax.rem(lax.div(q, cols), frames)
    target = frame * (2 * cols) + 2 * lax.rem(q, cols) + lax.div(q, width)
    spread[...] = jnp.where(o == target, 1.0, 0.0).astype(BF16)

    loads[0].wait()
    loads[1].wait()
    gain1 = g1[...].astype(F32).reshape(1, C)
    own_first = normed_silu(lat[...].astype(F32).reshape(width, C), gain1)
    rows_in[REACH] = packed(own_first, cols)

    rows_near = 1 + jnp.minimum(r, REACH) + jnp.minimum(R - 1 - r, REACH)
    pl.semaphore_wait(barrier, rows_near * T - 1)

    side = 1 - 2 * lax.rem(r, 2)

    def row_copy(d):
        slot = REACH - d
        return pltpu.make_async_remote_copy(
            src_ref=rows_in.at[REACH], dst_ref=rows_in.at[slot], send_sem=x1_send,
            recv_sem=x1_recv.at[slot - jnp.where(slot > REACH, 1, 0)],
            device_id={"rows": r + d}, device_id_type=MESH,
        )

    for d in (side, 2 * side, -2 * side, -side):
        pl.when(there(d))(lambda d=d: row_copy(d).start())

    def relay(slot):
        return pltpu.make_async_remote_copy(
            src_ref=rows_in.at[slot], dst_ref=hist.at[slot], send_sem=rl_send,
            recv_sem=rl_recv.at[slot], device_id={"tm": t + 1}, device_id_type=MESH,
        )

    gives = t < T - 1
    takes = t > 0
    pl.when(gives)(lambda: relay(REACH).start())

    stages = stages_of(R)

    def tell(i):
        for d in (stages[i], -stages[i]):
            pl.when(there(d))(
                lambda d=d: pl.semaphore_signal(
                    known.at[i], inc=1, device_id={"rows": r + d}, device_id_type=MESH
                )
            )

    def hear(i):
        d = stages[i]
        pl.when(jnp.logical_or(there(d), there(-d)))(
            lambda: pl.semaphore_wait(known.at[i], jnp.where(jnp.logical_and(there(d), there(-d)), 2, 1))
        )

    if stages:
        tell(0)

    def two_rows(row):
        rest = jnp.concatenate([row[:, LANES:C], jnp.zeros((1, 2 * LANES - C), F32)], axis=1)
        return jnp.concatenate([row[:, 0:LANES], rest], axis=0)

    pk_first[...] = two_rows(peak_of(own_first.astype(BF16).astype(F32)))

    def contribute(source, past_frames):
        f0, f1 = frames_of(source.at[REACH])
        both = jnp.concatenate([f0, f1], axis=0)
        tap = 0 if past_frames else 2
        for at in range(3):
            j = 2 - at
            for k in range(3):
                main = dot(both, w1[(tap * 3 + j) * 3 + k])
                extra = dot(f1 if past_frames else f0, w1[(3 + j) * 3 + k])
                early, late = main[0:cols], main[cols:]
                if past_frames:
                    acc[k, at, 0:cols] += early + extra
                    acc[k, at, cols:] += late
                else:
                    acc[k, at, 0:cols] = early
                    acc[k, at, cols:] = late + extra

    def contribute_side(source, s, past_frames):
        n0, n1 = frames_of(source.at[REACH + s])
        f0, f1 = frames_of(source.at[REACH + 2 * s])
        near_rows = jnp.concatenate([n0, n1], axis=0)
        all_rows = jnp.concatenate([n0, n1, f0, f1], axis=0)
        near_one, far_one = (n1, f1) if past_frames else (n0, f0)
        ones = jnp.concatenate([near_one, far_one], axis=0)
        tap = 0 if past_frames else 2
        mixed = slice(0, cols) if past_frames else slice(cols, width)
        for k in range(3):
            main = dot(all_rows, w1[(tap * 3 + 1 + s) * 3 + k])
            extra = dot(ones, w1[(3 + 1 + s) * 3 + k])
            acc[k, 1] += main[0:width]
            acc[k, 1, mixed] += extra[0:cols]
            acc[k, 1 + s] += main[width:] + dot(near_rows, w1[(tap * 3 + 1) * 3 + k])
            acc[k, 1 + s, mixed] += extra[cols:] + dot(near_one, w1[(3 + 1) * 3 + k])

    loads[3].wait()
    loads[4].start()
    loads[5].start()
    contribute(rows_in, False)

    def await_row(d):
        @pl.when(there(d))
        def _():
            row_copy(-d).wait_recv()
            pl.when(gives)(lambda: relay(REACH + d).start())

    def await_past(d):
        pl.when(there(d))(lambda: relay(REACH + d).wait_recv())

    lane0 = lax.rem(lax.broadcasted_iota(jnp.int32, (width, 1), 0), cols)

    def shifted_sum(left, middle, right):
        left = jnp.where(lane0 == 0, 0.0, pltpu.roll(left, 1, 0))
        right = jnp.where(lane0 == cols - 1, 0.0, pltpu.roll(right, width - 1, 0))
        return left + middle + right

    def activate(slot):
        o = (side, 0, -side)[slot]
        if slot == 1:
            activate_row(slot, o)
        else:
            pl.when(there(o))(lambda: activate_row(slot, o))

    def activate_row(slot, o):
        at = 1 + o
        hidden = shifted_sum(acc[0, at], acc[1, at], acc[2, at]).astype(BF16).astype(F32)
        values = normed_silu(hidden, gain2).astype(BF16)
        if slot == 1:
            pk_second[...] = two_rows(peak_of(values.astype(F32)))
        second[slot, :, 0:C] = values

    def gift_copy():
        return pltpu.make_async_remote_copy(
            src_ref=gift_out, dst_ref=gift, send_sem=s_send, recv_sem=s_recv,
            device_id={"tm": t + 1}, device_id_type=MESH,
        )

    loads[2].wait()
    gain2 = g2[...].astype(F32).reshape(1, C)

    def second_conv(past_frames):
        rows = [second[slot] for slot in range(3)]
        both = jnp.concatenate(rows, axis=1)
        one = jnp.concatenate([row[cols:] if past_frames else row[0:cols] for row in rows], axis=1)

        def taps_at(i, k):
            return jnp.concatenate([w2[(i * 3 + 1 + o) * 3 + k] for o in (side, 0, -side)], axis=0)

        sums = []
        for k in range(3):
            main = dot(both, taps_at(0 if past_frames else 2, k))
            extra = dot(one, taps_at(1, k))
            if past_frames:
                sums.append(jnp.concatenate([main[0:cols] + extra, main[cols:]], axis=0))
            else:
                sums.append(jnp.concatenate([main[0:cols], main[cols:] + extra], axis=0))
        if past_frames:
            gift_out[...] = shifted_sum(*sums).astype(BF16)
        else:
            mix[...] = shifted_sum(*sums)

    def meet():
        for i in range(1, len(stages)):
            hear(i - 1)
            tell(i)

    last_core = t == T - 1
    alone = 2 * r >= R
    alone_rows = R - (R + 1) // 2
    sources = R + alone_rows * (T - 1)
    slot = jnp.where(last_core, r, R + (r - (R - alone_rows)) * (T - 1) + t)

    def peak_copy(peer):
        return pltpu.make_async_remote_copy(
            src_ref=pk_send, dst_ref=pk_recv.at[slot], send_sem=pk_ssem, recv_sem=pk_rsem,
            device_id={"rows": peer // T, "tm": lax.rem(peer, T)}, device_id_type=MESH,
        )

    def send_peaks():
        def step(i, carry):
            p = jnp.where(2 * r >= R, i, n - 2 - i)
            peak_copy(jnp.where(p >= me, p + 1, p)).start()
            return carry

        lax.fori_loop(0, n - 1, step, 0, unroll=n <= 16)

    def pass_peaks():
        return pltpu.make_async_remote_copy(
            src_ref=pk_send, dst_ref=pk_past, send_sem=pk_ssem, recv_sem=pp_rsem,
            device_id={"tm": t + 1}, device_id_type=MESH,
        )

    def peaks_of(count):
        return pltpu.make_async_remote_copy(
            src_ref=pk_recv.at[pl.ds(0, count)], dst_ref=pk_recv.at[pl.ds(0, count)],
            send_sem=pk_ssem, recv_sem=pk_rsem,
            device_id={"rows": r, "tm": lax.rem(t + 1, T)}, device_id_type=MESH,
        )

    shares = jnp.logical_or(last_core, alone)

    def heard():
        if stages:
            hear(len(stages) - 1)

    def beside(source, s, past_frames):
        pl.when(there(s))(lambda: contribute_side(source, s, past_frames))

    @pl.when(jnp.logical_not(takes))
    def _():
        await_row(-2)
        meet()
        await_row(side)
        await_row(2)
        beside(rows_in, side, False)
        activate(0)
        await_row(-side)
        beside(rows_in, -side, False)
        activate(1)
        activate(2)
        loads[4].wait()

        @pl.when(gives)
        def _():
            second_conv(True)
            gift_copy().start()

        second_conv(False)

    @pl.when(takes)
    def _():
        relay(REACH).wait_recv()
        contribute(hist, True)
        meet()
        await_row(-2)
        await_row(side)
        await_row(2)
        beside(rows_in, side, False)
        await_row(-side)
        beside(rows_in, -side, False)
        loads[4].wait()
        heard()
        await_past(-2)
        await_past(side)
        await_past(2)
        beside(hist, side, True)
        activate(0)
        await_past(-side)
        beside(hist, -side, True)
        activate(1)
        activate(2)
        second_conv(False)
        gift_copy().wait_recv()

    block = lat[...].astype(F32).reshape(width, C) + mix[...] + gift[...].astype(F32)
    block = block.astype(BF16)
    wide_block = block.astype(F32)
    merged[1] = packed(wide_block, cols)
    peaks = jnp.concatenate([pk_first[...], pk_second[...], two_rows(peak_of(wide_block))], axis=0)
    def edge_copy(d):
        slot = 1 - d
        return pltpu.make_async_remote_copy(
            src_ref=merged.at[1], dst_ref=merged.at[slot], send_sem=x3_send,
            recv_sem=x3_recv.at[slot // 2], device_id={"rows": r + d}, device_id_type=MESH,
        )

    def send_edges():
        for d in (side, -side):
            pl.when(there(d))(lambda d=d: edge_copy(d).start())

    def with_past():
        @pl.when(jnp.logical_and(takes, jnp.logical_not(alone)))
        def _():
            pass_peaks().wait_recv()
            pk_send[...] = jnp.maximum(pk_send[...].astype(F32), pk_past[...].astype(F32)).astype(BF16)

    pk_send[...] = peaks.astype(BF16)
    pl.when(jnp.logical_not(takes))(heard)
    low = jnp.logical_and(2 * r < R, takes)

    @pl.when(low)
    def _():
        send_edges()

    with_past()

    @pl.when(shares)
    def _():
        pk_recv[slot] = pk_send[...]
        send_peaks()

    @pl.when(jnp.logical_not(shares))
    def _():
        pass_peaks().start()

    @pl.when(jnp.logical_not(low))
    def _():
        send_edges()

    loads[5].wait()
    C2 = dec_ref.shape[2]
    own = dot_nt(up[...], block).reshape(3, 3, C2, width)
    base[0] = own[1] + own[2]
    base[1] = own[0] + own[1]
    lane = lax.rem(lax.broadcasted_iota(jnp.int32, (C2, width), 1), cols)

    def columns(sums):
        from_left = jnp.where(lane == 0, 0.0, pltpu.roll(sums[0], 1, 1))
        from_right = jnp.where(lane == cols - 1, 0.0, pltpu.roll(sums[2], width - 1, 1))
        even = from_left + sums[1] + sums[2]
        odd = sums[0] + sums[1] + from_right
        return jnp.concatenate([even, odd], axis=1).astype(BF16)

    def decode_row(half):
        f0, f1 = frames_of(merged.at[2 * half])
        rows = jnp.concatenate([f0, f1], axis=0)[:, 0:C]
        taps = up[half * 6 * C2 : (half * 6 + 3) * C2]
        sums = base[half] + dot_nt(taps, rows).reshape(3, C2, width)
        wide = dot(columns(sums), spread[...]).astype(BF16)
        for f in range(frames):
            dec_ref[f, half] = wide[:, f * 2 * cols : (f + 1) * 2 * cols]

    for d in (-1, 1):
        pl.when(there(d))(lambda d=d: edge_copy(-d).wait_recv())
        decode_row((1 + d) // 2)

    pl.when(shares)(lambda: peaks_of(sources - 1).wait_recv())
    pl.when(jnp.logical_not(shares))(lambda: peaks_of(sources).wait_recv())

    def take_peak(i, best):
        return jnp.maximum(best, pk_recv[i].astype(F32))

    best = lax.fori_loop(1, sources, take_peak, pk_recv[0].astype(F32), unroll=n <= 16)
    for i in range(3):
        peaks_ref[i : i + 1, 0:LANES] = best[2 * i : 2 * i + 1, :]
        peaks_ref[i : i + 1, LANES:C] = best[2 * i + 1 : 2 * i + 2, 0 : C - LANES]

    def sent(ref, sem, count, most):
        for c in range(1, most + 1):
            pl.when(count == c)(
                lambda c=c: pltpu.make_async_remote_copy(
                    src_ref=ref.at[pl.ds(0, c)], dst_ref=ref.at[pl.ds(0, c)], send_sem=sem, recv_sem=sem,
                    device_id={"rows": r, "tm": lax.rem(t + 1, T)}, device_id_type=MESH,
                ).wait_send()
            )

    sent(rows_in, x1_send, rows_near - 1, 2 * REACH)
    sent(merged, x3_send, jnp.minimum(r, 1) + jnp.minimum(R - 1 - r, 1), 2)

    @pl.when(gives)
    def _():
        sent(rows_in, rl_send, rows_near, 2 * REACH + 1)
        gift_copy().wait_send()

    pl.when(shares)(lambda: peaks_of(n - 1).wait_send())
    pl.when(jnp.logical_not(shares))(lambda: pass_peaks().wait_send())


def per_device(latent, gain_first, conv_first, gain_second, conv_second, conv_up):
    frames, rows, cols, C = latent.shape
    R, T = lax.axis_size("rows"), lax.axis_size("tm")
    C2 = conv_up.shape[2]
    n = R * T
    if rows != 1 or frames != 2 or 2 * C != 3 * LANES:
        raise ValueError("unsupported block")
    depth = 2 * LANES
    taps = conv_first.shape[0] * conv_first.shape[1] * conv_first.shape[2]
    vmem = pl.BlockSpec(memory_space=pltpu.VMEM)
    hbm = pl.BlockSpec(memory_space=pltpu.HBM)
    dma = pltpu.SemaphoreType.DMA
    span = 2 * REACH + 1
    width = frames * cols
    decoded, peaks = pl.pallas_call(
        functools.partial(kernel, R, T),
        out_shape=(
            pltpu.VMEM((frames, 2 * rows, C2, 2 * cols), BF16),
            pltpu.VMEM((3, C), F32),
        ),
        in_specs=[hbm] * 6,
        out_specs=(vmem, vmem),
        scratch_shapes=[
            pltpu.VMEM((frames, cols, C), BF16),
            pltpu.VMEM((C,), BF16),
            pltpu.VMEM((C,), BF16),
            pltpu.VMEM((span, 3, cols, LANES), BF16),
            pltpu.VMEM((span, 3, cols, LANES), BF16),
            pltpu.VMEM((3, 3, width, C), F32),
            pltpu.VMEM((width, C), F32),
            pltpu.VMEM((width, C), BF16),
            pltpu.VMEM((width, C), BF16),
            pltpu.VMEM((2, 3, C2, width), F32),
            pltpu.VMEM((3, width, depth), BF16),
            pltpu.VMEM((taps, depth, C), BF16),
            pltpu.VMEM((taps, depth, C), BF16),
            pltpu.VMEM((9 * C2, C), BF16),
            pltpu.VMEM((3, 3, cols, LANES), BF16),
            pltpu.VMEM((6, LANES), BF16),
            pltpu.VMEM((n + R, 6, LANES), BF16),
            pltpu.VMEM((6, LANES), BF16),
            pltpu.VMEM((2, LANES), F32),
            pltpu.VMEM((2, LANES), F32),
            dma((6,)),
            dma,
            dma((span - 1,)),
            dma,
            dma((span,)),
            dma,
            dma,
            dma,
            dma((2,)),
            dma,
            dma,
            dma,
            pltpu.SemaphoreType.REGULAR((max(1, len(stages_of(R))),)),
            pltpu.VMEM((2 * width, 2 * width), BF16),
        ],
        compiler_params=pltpu.CompilerParams(collective_id=0, has_side_effects=True, vmem_limit_bytes=54 * 2**20),
    )(
        latent.reshape(frames, cols, C),
        gain_first,
        conv_first.reshape(taps, C, C),
        gain_second,
        conv_second.reshape(taps, C, C),
        conv_up.reshape(9 * C2, C),
    )
    return pl.pallas_call(
        finish,
        out_shape=(
            jax.ShapeDtypeStruct(decoded.shape, BF16),
            jax.ShapeDtypeStruct(peaks.shape, F32),
        ),
        in_specs=[vmem, vmem],
        out_specs=(hbm, hbm),
        scratch_shapes=[dma((2,))],
        compiler_params=pltpu.CompilerParams(vmem_limit_bytes=2**20),
    )(decoded, peaks)


def solution(mesh):
    return jax.shard_map(
        per_device,
        mesh=mesh,
        in_specs=(P(("clip", "tm"), "rows", None, None), P(), P(), P(), P(), P()),
        out_specs=(P(("clip", "tm"), "rows", None, None), P("clip", None)),
        check_vma=False,
    )
```
